32 devices in a mesh: gx: 4 (over y, x), gy: 8 (over z, core).
Axes of the slice: x: 2, y: 2, z: 4, core: 2. Of those that a mesh axis runs over, the one named last changes fastest.
Arguments:
- facets: float32 [2048, 12, 128], P(('gx', 'gy')), may hold values from -6 to 6
- owner: int32 [2048, 1], P(('gx', 'gy')), may hold values from 0 to 31; in each aligned block of 64 rows (0 to 63, 64 to 127, ...) at most 4 rows name the same one
- ghosts: int32 [32, 16], P(('gx', 'gy')), may hold values from 0 to 2047, as said below
- ghost_count: int32 [32], P(('gx', 'gy')), may hold values from 1 to 16, 256 in all
- nodes: float32 [3, 16384], P(None, ('gx', 'gy')), may hold values from -6 to 6
- cand: int32 [4, 16384], P(None, ('gx', 'gy')), may hold values from 0 to 15
Outputs:
- own_gap: float32 [16384], P(('gx', 'gy'))
- ghost_gap: float32 [16384], P(('gx', 'gy'))
The draws below stay inside these ranges and needn't reach their ends.
Inputs may be any that keep to these rules, and one draw needn't show every extreme that they name: Among the 64 blocks of one element-order device at most 4 have the same owner, and some owner reaches 4; every partition owns at least one block. `ghosts`: each row holds 16 distinct block ids. The blocks of element-order device h are h * 64 to h * 64 + 63; in every row exactly one device holds 2 of the entries and every other device holds at most one.
All inputs are finite; a program needn't handle non-finite values. No bound on the sum of `ghost_count` on one device may be relied on, other than what follows from the above.
Results may differ from the reference program's by a relative error of at most 0.0003.
Values sent between devices are 32-bit elements; how exact they have to be, the bound alone decides.
No kernel may reach another device: no remote copies, remote signals or barrier semaphores. Data moves between devices by JAX's collectives and lax.ppermute only.
A program may use at most 64 MiB of HBM per device.

```python
import math
import jax
import jax.numpy as jnp
import numpy as np
from jax import lax

FB = 128
BPD = 64
ND = 512
CAP = 4
GH = 16
NC = 4
PARTS_SIZE = 32
NB = 2048
NODES = 16384
N_GX = 4
N_GY = 8


def draw_ghosts(key, part):

    def one_row(row_key):
        subkeys = jax.random.split(row_key, 4)
        holders = jax.random.permutation(subkeys[0], PARTS_SIZE)[:GH - 1].astype(jnp.int32)
        entry_holder = jnp.concatenate([holders[:1], holders])
        offsets = jax.random.randint(subkeys[1], (GH,), 0, BPD).astype(jnp.int32)
        stride = jax.random.randint(subkeys[2], (), 1, BPD).astype(jnp.int32)
        partner = (offsets[0] + stride) % BPD
        offsets = offsets.at[1].set(partner)
        block_ids = entry_holder * BPD + offsets
        shuffle = jax.random.permutation(subkeys[3], GH)
        return block_ids[shuffle]
    return jax.vmap(one_row)(jax.random.split(jax.random.fold_in(key, 11), PARTS_SIZE)).astype(jnp.int32)


def plant(drawn, own_key, least, top_value):
    place = [jax.random.randint(jax.random.fold_in(own_key, axis), (), 0, length) for axis, length in enumerate(drawn.shape)]
    widest = drawn.shape.index(max(drawn.shape))
    neighbour = place[:widest] + [(place[widest] + 1) % drawn.shape[widest]] + place[widest + 1:]
    return drawn.at[tuple(place)].set(least).at[tuple(neighbour)].set(top_value)


def block_scale(key, extent, cuts, low, largest):
    factor_of, own = 1.0, jax.random.fold_in(key, 6)
    for position, shards_of in cuts:
        heights = jnp.exp(jax.random.uniform(jax.random.fold_in(own, position), (shards_of,), jnp.float32, low / len(cuts), largest / len(cuts)))
        factor_of = factor_of * jnp.repeat(heights, extent[position] // shards_of).reshape([-1 if axis == position else 1 for axis in range(len(extent))])
    return factor_of


def profile(amount, total, bound, lean):
    loads = [(1 << 20) // math.isqrt(rank ** lean) + 1 for rank in range(2, amount + 1)]
    spare, given = total - bound - (amount - 1), [1] * (amount - 1)
    while spare > 0:
        candidates = [i for i in range(amount - 1) if given[i] < bound]
        whole, budget = sum([loads[i] for i in candidates]), spare
        for i in candidates:
            addition = min(bound - given[i], max(1, budget * loads[i] // whole), spare)
            given[i] = given[i] + addition
            spare = spare - addition
    return np.array([bound] + given)


def ragged_sizes(own_key, number_of, total, most, skew):
    if number_of == 2:
        one = jax.random.randint(own_key, (), max(1, total - most), min(most, total - 1) + 1)
        return jnp.stack([one, total - one])
    sizes = jnp.asarray(profile(number_of, total, most, skew), jnp.int32)
    pairs = (number_of - 1) // 2
    giver, sink = sizes[1:1 + 2 * pairs:2], sizes[2:2 + 2 * pairs:2]
    margin = jnp.minimum(giver - 1, most - sink)
    passed = jax.random.randint(jax.random.fold_in(own_key, 1), (pairs,), 0, 1 << 20) % (margin + 1)
    sizes = sizes.at[1:1 + 2 * pairs:2].set(giver - passed).at[2:2 + 2 * pairs:2].set(sink + passed)
    return sizes[jax.random.permutation(jax.random.fold_in(own_key, 2), number_of)]


def assign_block(key, own, number, rows, count, top, reach, lean):
    ranking = jax.random.permutation(key, count)
    heavy_load, ordinary = portions_of(count, rows * top, reach, lean, True), portions_of(count, rows * top, reach, lean, False)
    places = jnp.arange(count)

    def named(lengths, rotation):
        used = int((lengths > 0).sum())
        fixed = max(1, used // 4)
        shifted = fixed + (places - fixed + rotation * (used - fixed)) % max(1, count - fixed)
        return jnp.zeros((count,), jnp.int32).at[ranking[jnp.where(places < fixed, places, shifted)]].set(jnp.asarray(lengths, jnp.int32))

    lengths = jnp.where(number % 4 == 0, named(heavy_load, number // 4), named(ordinary, number - number // 4 - 1))
    mixed = jax.random.permutation(jax.random.fold_in(own, 3), count)
    source_of, taker = mixed[0:count // 2 * 2:2], mixed[1:count // 2 * 2:2]
    slack = jnp.minimum(lengths[source_of] - 1, reach - lengths[taker]) // 2
    slack = jnp.where((source_of == ranking[0]) | (taker == ranking[0]) | (lengths[taker] == 0), 0, jnp.maximum(slack, 0))
    shifted = jax.random.randint(jax.random.fold_in(own, 4), (count // 2,), 0, 1 << 20) % (slack + 1)
    lengths = lengths.at[source_of].add(-shifted).at[taker].add(shifted)
    items = jnp.searchsorted(jnp.cumsum(lengths), jnp.arange(rows * top), side="right").astype(jnp.int32)
    grid = items.reshape(top, rows).T
    grid = grid[jax.random.permutation(jax.random.fold_in(own, 1), rows)]
    rotation = jax.random.randint(jax.random.fold_in(own, 2), (rows, 1), 0, top)
    return jnp.take_along_axis(grid, (jnp.arange(top)[None, :] + rotation) % top, axis=1)


def portions_of(amount, total, most, lean, full):
    portions = [(1 << 20) // math.isqrt(rank ** lean) + 1 for rank in range(1, amount + 1)]
    largest = most if full else min(most, max(-(-total // amount), total * portions[0] // sum(portions)))
    least = 1 if total - largest >= amount - 1 else 0
    counts, surplus = [largest] + [least] * (amount - 1), total - largest - least * (amount - 1)
    while surplus > 0:
        free = [i for i in range(1, amount) if counts[i] < largest] or [i for i in range(1, amount) if counts[i] < most]
        pool, remaining = sum([portions[i] for i in free]), surplus
        for i in free:
            addition = min(most - counts[i], max(1, remaining * portions[i] // pool), surplus)
            counts[i] = counts[i] + addition
            surplus = surplus - addition
    return np.array(counts)


def normal_values(rng, shape, deviation, most, cuts=(), kind=jnp.bfloat16):
    values = deviation * jax.random.normal(rng, shape, jnp.float32)
    if cuts:
        values = values * block_scale(rng, shape, cuts, -0.22, 0.18)
    return jnp.clip(values, -most, most).astype(kind)


def setup_inputs(seed: int = 0) -> dict:
    key_of = jax.random.split(jax.random.key(seed), 7)
    facets = normal_values(key_of[0], (NB, 12, FB), 1.0, 6.0, ((0, 32),), jnp.float32)
    owner_keys = jax.random.split(jax.random.fold_in(key_of[1], 1), NB // BPD)
    owner_turns = jax.random.permutation(jax.random.fold_in(key_of[1], 3), NB // BPD)
    owner = jax.vmap(lambda own, number: assign_block(jax.random.fold_in(key_of[1], 2), own, number, BPD, PARTS_SIZE, 1, CAP, 2))(owner_keys, owner_turns).reshape((NB, 1))
    ghosts = draw_ghosts(jax.random.fold_in(key_of[6], 71), 0)
    ghost_count = ragged_sizes(key_of[3], PARTS_SIZE, PARTS_SIZE * GH // 2, GH, 2).astype(jnp.int32)
    nodes = normal_values(key_of[4], (3, NODES), 1.0, 6.0, ((1, 32),), jnp.float32)
    cand = plant(jax.random.randint(key_of[5], (NC, NODES), 0, GH), jax.random.fold_in(key_of[5], 1), 0, GH - 1).astype(jnp.int32)
    return dict(facets=facets, owner=owner, ghosts=ghosts, ghost_count=ghost_count, nodes=nodes, cand=cand)


far_gap = 10.0
penalty = 1.0e30


def facet_features(blocks, absent):
    vertex_a = blocks[:, 0:3]
    vertex_b = blocks[:, 3:6]
    vertex_c = blocks[:, 6:9]
    normal = blocks[:, 9:12]
    centre = (vertex_a + vertex_b + vertex_c) / 3.0
    spread = jnp.sum(vertex_a * vertex_a + vertex_b * vertex_b + vertex_c * vertex_c, axis=1) / 3.0
    offset = spread - jnp.sum(normal * vertex_a, axis=1) + penalty * absent[:, None]
    linear = normal - 2.0 * centre
    unit_row = jnp.ones_like(offset)
    stacked = jnp.concatenate([linear, unit_row[:, None], offset[:, None]], axis=1)
    return jnp.moveaxis(stacked, 1, 0).reshape(5, -1)


def node_features(points):
    square = jnp.sum(points * points, axis=0, keepdims=True)
    return jnp.concatenate([points, square, jnp.ones_like(square)], axis=0)


def pair_gaps(node_feat, facet_feat):
    return lax.dot_general(node_feat, facet_feat, (((0,), (0,)), ((), ())), precision=lax.Precision.HIGHEST, preferred_element_type=jnp.float32)


def reference(facets, owner, ghosts, ghost_count, nodes, cand):
    part_count = N_GX * N_GY
    slot_count = part_count * CAP
    target = owner[:, 0]
    per_part = jnp.moveaxis(nodes.reshape(3, part_count, ND), 1, 0)
    cand_part = jnp.moveaxis(cand.reshape(NC, part_count, ND), 1, 0)
    entries = jnp.arange(GH, dtype=jnp.int32)

    def one_part(operands):
        index, points, chosen, wanted, limit = operands
        node_feat = node_features(points)
        owned = target == index
        ordering = jnp.argsort(jnp.where(owned, 0, 1).astype(jnp.int32), stable=True)[:slot_count]
        absent = jnp.where(owned[ordering], 0.0, 1.0).astype(jnp.float32)
        own_min = jnp.min(pair_gaps(node_feat, facet_features(facets[ordering], absent)), axis=1)
        fetched = facets[wanted]
        gap_block = pair_gaps(node_feat, facet_features(fetched, jnp.zeros((GH,), jnp.float32))).reshape(ND, GH, FB)
        active = jnp.any((chosen[:, :, None] == entries[None, None, :]) & (entries[None, None, :] < limit), axis=0)
        ghost_min = jnp.minimum(far_gap, jnp.min(jnp.where(active[:, :, None], gap_block, penalty), axis=(1, 2)))
        return own_min, ghost_min

    own_min, ghost_min = lax.map(one_part, (jnp.arange(part_count, dtype=jnp.int32), per_part, cand_part, ghosts, ghost_count))
    return own_min.reshape(part_count * ND), ghost_min.reshape(part_count * ND)
```

```python
import jax
import jax.numpy as jnp
from jax import lax
from jax.experimental import pallas as pl
from jax.experimental.pallas import tpu as pltpu
from jax.sharding import PartitionSpec as P

CAP = 4
GC = 2
FEAT = 4
OWN_ROWS = CAP * FEAT
SEND_ROWS = OWN_ROWS + 1
REPLY_ROWS = GC * FEAT
AXES = ("gx", "gy")

far_gap = 10.0
penalty = 1e30


def split3(value):
    high = value.astype(jnp.bfloat16)
    rest = value - high.astype(jnp.float32)
    middle = rest.astype(jnp.bfloat16)
    low = (rest - middle.astype(jnp.float32)).astype(jnp.bfloat16)
    return high, middle, low


def to_one(flag):
    return jnp.where(flag, 1.0, 0.0)


def pack_kernel(facets_ref, owner_ref, ghosts_ref, out_ref, feat_ref):
    _, blocks, width = facets_ref.shape
    parts = out_ref.shape[0] // SEND_ROWS
    ax, ay, az, bx, by, bz, cx, cy, cz, nx, ny, nz = [facets_ref[i] for i in range(12)]
    third = 1.0 / 3.0
    squares = lambda u, v, w: u * u + v * v + w * w
    spread = (squares(ax, bx, cx) + squares(ay, by, cy) + squares(az, bz, cz)) * third
    offset = spread - (nx * ax + ny * ay + nz * az)
    feats = [n - (2.0 * third) * (a + b + c) for n, a, b, c in ((nx, ax, bx, cx), (ny, ay, by, cy), (nz, az, bz, cz))]
    feats.append(offset)
    splits = [split3(f) for f in feats]
    table = jnp.concatenate(
        [jnp.concatenate([splits[c][i] for c in range(FEAT)], axis=1) for i in range(3)], axis=0
    )
    feat_ref[...] = table

    owner_row = owner_ref[...]
    row_id = lax.broadcasted_iota(jnp.int32, (blocks, blocks), 0)
    col_id = lax.broadcasted_iota(jnp.int32, (blocks, blocks), 1)
    owner_col = jnp.sum(jnp.where(row_id == col_id, owner_row, 0), axis=1, keepdims=True)
    earlier = (owner_col == owner_row) & (row_id < col_id)
    rank = jnp.sum(jnp.where(earlier, 1, 0), axis=0, keepdims=True)
    part_id = lax.broadcasted_iota(jnp.int32, (parts, blocks), 0)
    mine = owner_row == part_id
    picks = [to_one(mine & (rank == s)) for s in range(CAP)]
    pick = jnp.concatenate(picks, axis=0).astype(jnp.bfloat16)
    placed = jnp.dot(jnp.concatenate([pick] * 3, axis=1), table, preferred_element_type=jnp.float32)
    for s in range(CAP):
        absent = 1.0 - jnp.sum(picks[s], axis=1, keepdims=True)
        for c in range(FEAT):
            piece = placed[s * parts : (s + 1) * parts, c * width : (c + 1) * width]
            if c == FEAT - 1:
                piece = piece + penalty * absent
            out_ref[pl.ds(s * FEAT + c, parts, stride=SEND_ROWS), :] = piece

    wanted = ghosts_ref[...]
    entries = wanted.shape[1]
    part_of = lax.broadcasted_iota(jnp.int32, (parts, entries), 0)
    entry = lax.broadcasted_iota(jnp.int32, (parts, entries), 1)
    holder = wanted // blocks
    local_row = wanted - holder * blocks
    held = part_of == holder
    first = jnp.min(jnp.where(held, entry, entries), axis=1, keepdims=True)
    last = jnp.max(jnp.where(held, entry, -1), axis=1, keepdims=True)
    row_first = jnp.sum(jnp.where(held & (entry == first), local_row, 0), axis=1, keepdims=True)
    row_last = jnp.sum(jnp.where(held & (entry == last), local_row, 0), axis=1, keepdims=True)
    lane = lax.broadcasted_iota(jnp.int32, (parts, width), 1)
    request = jnp.where(lane == 0, row_first, jnp.where(lane == 1, row_last, 0))
    out_ref[pl.ds(OWN_ROWS, parts, stride=SEND_ROWS), :] = request.astype(jnp.float32)


def select_kernel(arrived_ref, feat_ref, out_ref):
    parts = arrived_ref.shape[0] // SEND_ROWS
    width = arrived_ref.shape[1]
    blocks = feat_ref.shape[0] // 3
    request = arrived_ref[pl.ds(OWN_ROWS, parts, stride=SEND_ROWS), :].astype(jnp.int32)
    block_id = lax.broadcasted_iota(jnp.int32, (parts, blocks), 1)
    pick = jnp.concatenate([to_one(request[:, s : s + 1] == block_id) for s in range(GC)], axis=0)
    pick = pick.astype(jnp.bfloat16)
    rows = jnp.dot(jnp.concatenate([pick] * 3, axis=1), feat_ref[...], preferred_element_type=jnp.float32)
    for s in range(GC):
        for c in range(FEAT):
            out_ref[pl.ds(s * FEAT + c, parts, stride=REPLY_ROWS), :] = rows[
                s * parts : (s + 1) * parts, c * width : (c + 1) * width
            ]


def own_kernel(arrived_ref, nodes_ref, out_ref, spread_ref, best_ref):
    parts = arrived_ref.shape[0] // SEND_ROWS
    width = arrived_ref.shape[1]
    count = nodes_ref.shape[1]
    for c in range(3):
        for g in range(count // width):
            row = nodes_ref[c : c + 1, g * width : (g + 1) * width]
            spread_ref[c, g * width : (g + 1) * width, :] = jnp.broadcast_to(row, (width, width)).T
    chunk = 64

    def one_chunk(j, carry):
        start = pl.multiple_of(j * chunk, chunk)
        x, y, z = [spread_ref[c, pl.ds(start, chunk), :] for c in range(3)]

        def one_source(d, best):
            base = d * SEND_ROWS
            for s in range(CAP):
                lx, ly, lz, off = [arrived_ref[pl.ds(base + s * FEAT + c, 1), :] for c in range(FEAT)]
                best = jnp.minimum(best, (x * lx + y * ly) + (z * lz + off))
            return best

        best_ref[pl.ds(start, chunk), :] = lax.fori_loop(
            0, parts, one_source, jnp.full((chunk, width), penalty, jnp.float32)
        )
        return carry

    lax.fori_loop(0, count // chunk, one_chunk, 0)
    for g in range(count // width):
        here = slice(g * width, (g + 1) * width)
        least = jnp.min(best_ref[here, :].T, axis=0, keepdims=True)
        px, py, pz = [nodes_ref[c : c + 1, here] for c in range(3)]
        out_ref[:, here] = least + (px * px + py * py + pz * pz)


def ghost_kernel(place_ref, limit_ref, reply_ref, nodes_ref, cand_ref, out_ref, got_ref, mask_ref):
    entries = place_ref.shape[0]
    width = reply_ref.shape[1]
    count = nodes_ref.shape[1]
    groups = count // width
    for e in range(entries):
        got_ref[e * FEAT : (e + 1) * FEAT, :] = reply_ref[pl.ds(place_ref[e], FEAT), :]
    entry = lax.broadcasted_iota(jnp.int32, (entries, count), 0)
    chosen = entry == cand_ref[0:1, :]
    for k in range(1, cand_ref.shape[0]):
        chosen = chosen | (entry == cand_ref[k : k + 1, :])
    mask_ref[...] = jnp.where(chosen & (entry < limit_ref[0]), -penalty, penalty)
    turned = got_ref[...].T
    points = [
        [jnp.broadcast_to(nodes_ref[c : c + 1, g * width : (g + 1) * width], (8, width)) for g in range(groups)]
        for c in range(3)
    ]
    total = [jnp.full((8, width), penalty, jnp.float32) for _ in range(groups)]
    for e in range(entries):
        best = [None] * groups
        for f in range(width // 8):
            lx, ly, lz, off = [
                jnp.broadcast_to(turned[f * 8 : (f + 1) * 8, e * FEAT + c : e * FEAT + c + 1], (8, width))
                for c in range(FEAT)
            ]
            for g in range(groups):
                gap = (points[0][g] * lx + points[1][g] * ly) + (points[2][g] * lz + off)
                best[g] = gap if best[g] is None else jnp.minimum(best[g], gap)
        for g in range(groups):
            masked = jnp.maximum(best[g], mask_ref[e : e + 1, g * width : (g + 1) * width])
            total[g] = jnp.minimum(total[g], masked)
    for g in range(groups):
        here = slice(g * width, (g + 1) * width)
        least = jnp.min(total[g], axis=0, keepdims=True)
        px, py, pz = [nodes_ref[c : c + 1, here] for c in range(3)]
        out_ref[:, here] = jnp.minimum(far_gap, least + (px * px + py * py + pz * pz))


def exchange(rows, parts):
    per_part = rows.shape[0] // parts
    shaped = rows.reshape(parts, per_part, 1, rows.shape[1])
    moved = lax.all_to_all(shaped, AXES, split_axis=0, concat_axis=0, tiled=True)
    return moved.reshape(rows.shape)


def local(facets, owner, ghosts, ghost_count, nodes, cand):
    parts = lax.axis_size(AXES)
    blocks, _, width = facets.shape
    count = nodes.shape[1]
    entries = ghosts.shape[1]
    f32 = jnp.float32
    outgoing, table = pl.pallas_call(
        pack_kernel,
        out_shape=(
            jax.ShapeDtypeStruct((parts * SEND_ROWS, width), f32),
            jax.ShapeDtypeStruct((3 * blocks, FEAT * width), jnp.bfloat16),
        ),
        name="pack",
    )(jnp.transpose(facets, (1, 0, 2)), owner.T, ghosts)
    arrived = exchange(outgoing, parts)
    answer = pl.pallas_call(
        select_kernel, out_shape=jax.ShapeDtypeStruct((parts * REPLY_ROWS, width), f32), name="select"
    )(arrived, table)
    reply = exchange(answer, parts)
    own_gap = pl.pallas_call(
        own_kernel,
        out_shape=jax.ShapeDtypeStruct((1, count), f32),
        scratch_shapes=[pltpu.VMEM((3, count, width), f32), pltpu.VMEM((count, width), f32)],
        name="own",
        cost_estimate=pl.CostEstimate(
            flops=7 * parts * CAP * width * count, bytes_accessed=parts * SEND_ROWS * width * 4, transcendentals=0
        ),
    )(arrived, nodes)
    wanted = ghosts[0]
    holder = wanted // blocks
    entry = jnp.arange(entries, dtype=jnp.int32)
    before = (holder[:, None] == holder[None, :]) & (entry[None, :] < entry[:, None])
    order = jnp.sum(before.astype(jnp.int32), axis=1, dtype=jnp.int32)
    place = (holder * GC + order) * FEAT
    smem = pl.BlockSpec(memory_space=pltpu.SMEM)
    vmem = pl.BlockSpec(memory_space=pltpu.VMEM)
    ghost_gap = pl.pallas_call(
        ghost_kernel,
        out_shape=jax.ShapeDtypeStruct((1, count), f32),
        in_specs=[smem, smem, vmem, vmem, vmem],
        scratch_shapes=[pltpu.VMEM((entries * FEAT, width), f32), pltpu.VMEM((entries, count), f32)],
        name="ghost",
    )(place, ghost_count, reply, nodes, cand)
    return own_gap.reshape(count), ghost_gap.reshape(count)


def solution(mesh):
    return jax.shard_map(
        local,
        mesh=mesh,
        in_specs=(
            P(AXES, None, None),
            P(AXES, None),
            P(AXES, None),
            P(AXES),
            P(None, AXES),
            P(None, AXES),
        ),
        out_specs=(P(AXES), P(AXES)),
        check_vma=False,
    )
```

```python
import functools

import jax
import jax.numpy as jnp
from jax import lax
from jax.experimental import pallas as pl
from jax.experimental.pallas import tpu as pltpu
from jax.sharding import PartitionSpec as P

CAP = 4
GC = 2
FEAT = 4
OWN_ROWS = CAP * FEAT
SEND_ROWS = OWN_ROWS + 1
REPLY_ROWS = GC * FEAT
AXES = ("gx", "gy")

far_gap = 10.0
penalty = 1e30


def split3(value):
    high = value.astype(jnp.bfloat16)
    rest = value - high.astype(jnp.float32)
    middle = rest.astype(jnp.bfloat16)
    low = (rest - middle.astype(jnp.float32)).astype(jnp.bfloat16)
    return high, middle, low


def to_one(flag):
    return jnp.where(flag, 1.0, 0.0)


def pack_kernel(facets_ref, owner_ref, ghosts_ref, out_ref, feat_ref):
    _, blocks, width = facets_ref.shape
    parts = out_ref.shape[0] // SEND_ROWS
    ax, ay, az, bx, by, bz, cx, cy, cz, nx, ny, nz = [facets_ref[i] for i in range(12)]
    third = 1.0 / 3.0
    squares = lambda u, v, w: u * u + v * v + w * w
    spread = (squares(ax, bx, cx) + squares(ay, by, cy) + squares(az, bz, cz)) * third
    offset = spread - (nx * ax + ny * ay + nz * az)
    feats = [n - (2.0 * third) * (a + b + c) for n, a, b, c in ((nx, ax, bx, cx), (ny, ay, by, cy), (nz, az, bz, cz))]
    feats.append(offset)
    splits = [split3(f) for f in feats]
    table = jnp.concatenate(
        [jnp.concatenate([splits[c][i] for c in range(FEAT)], axis=1) for i in range(3)], axis=0
    )
    feat_ref[...] = table

    owner_row = owner_ref[...]
    row_id = lax.broadcasted_iota(jnp.int32, (blocks, blocks), 0)
    col_id = lax.broadcasted_iota(jnp.int32, (blocks, blocks), 1)
    owner_col = jnp.sum(jnp.where(row_id == col_id, owner_row, 0), axis=1, keepdims=True)
    earlier = (owner_col == owner_row) & (row_id < col_id)
    rank = jnp.sum(jnp.where(earlier, 1, 0), axis=0, keepdims=True)
    part_id = lax.broadcasted_iota(jnp.int32, (parts, blocks), 0)
    mine = owner_row == part_id
    picks = [to_one(mine & (rank == s)) for s in range(CAP)]
    pick = jnp.concatenate(picks, axis=0).astype(jnp.bfloat16)
    placed = jnp.dot(jnp.concatenate([pick] * 3, axis=1), table, preferred_element_type=jnp.float32)
    for s in range(CAP):
        absent = 1.0 - jnp.sum(picks[s], axis=1, keepdims=True)
        for c in range(FEAT):
            piece = placed[s * parts : (s + 1) * parts, c * width : (c + 1) * width]
            if c == FEAT - 1:
                piece = piece + penalty * absent
            out_ref[pl.ds(s * FEAT + c, parts, stride=SEND_ROWS), :] = piece

    wanted = ghosts_ref[...]
    entries = wanted.shape[1]
    part_of = lax.broadcasted_iota(jnp.int32, (parts, entries), 0)
    entry = lax.broadcasted_iota(jnp.int32, (parts, entries), 1)
    holder = wanted // blocks
    local_row = wanted - holder * blocks
    held = part_of == holder
    first = jnp.min(jnp.where(held, entry, entries), axis=1, keepdims=True)
    last = jnp.max(jnp.where(held, entry, -1), axis=1, keepdims=True)
    row_first = jnp.sum(jnp.where(held & (entry == first), local_row, 0), axis=1, keepdims=True)
    row_last = jnp.sum(jnp.where(held & (entry == last), local_row, 0), axis=1, keepdims=True)
    lane = lax.broadcasted_iota(jnp.int32, (parts, width), 1)
    request = jnp.where(lane == 0, row_first, jnp.where(lane == 1, row_last, 0))
    out_ref[pl.ds(OWN_ROWS, parts, stride=SEND_ROWS), :] = request.astype(jnp.float32)


def select_kernel(arrived_ref, feat_ref, out_ref):
    parts = arrived_ref.shape[0] // SEND_ROWS
    width = arrived_ref.shape[1]
    blocks = feat_ref.shape[0] // 3
    request = arrived_ref[pl.ds(OWN_ROWS, parts, stride=SEND_ROWS), :].astype(jnp.int32)
    block_id = lax.broadcasted_iota(jnp.int32, (parts, blocks), 1)
    pick = jnp.concatenate([to_one(request[:, s : s + 1] == block_id) for s in range(GC)], axis=0)
    pick = pick.astype(jnp.bfloat16)
    rows = jnp.dot(jnp.concatenate([pick] * 3, axis=1), feat_ref[...], preferred_element_type=jnp.float32)
    for s in range(GC):
        for c in range(FEAT):
            out_ref[pl.ds(s * FEAT + c, parts, stride=REPLY_ROWS), :] = rows[
                s * parts : (s + 1) * parts, c * width : (c + 1) * width
            ]


def stack_terms(high, middle, low):
    return [high, high, high, middle, middle, low]


def point_terms(points):
    four = jnp.concatenate([points, jnp.ones_like(points[0:1])], axis=0)
    high, middle, low = [t.astype(jnp.float32) for t in split3(jnp.concatenate([four, four], axis=0))]
    return [high, middle, low, high, middle, high]


def own_kernel(limit_ref, arrived_ref, nodes_ref, cand_ref, out_ref, left_ref, spread_ref, best_ref):
    parts = arrived_ref.shape[0] // SEND_ROWS
    width = arrived_ref.shape[1]
    count = nodes_ref.shape[1]
    half = count // 2
    entries = left_ref.shape[1] - 6 * 2 * FEAT
    entry = lax.broadcasted_iota(jnp.int32, (entries, count), 0)
    chosen = entry == cand_ref[0:1, :]
    for k in range(1, cand_ref.shape[0]):
        chosen = chosen | (entry == cand_ref[k : k + 1, :])
    mask = jnp.where(chosen & (entry < limit_ref[0]), 0.0, penalty)
    left = jnp.concatenate(point_terms(nodes_ref[...]) + [mask], axis=0).T.astype(jnp.bfloat16)
    left_ref[...] = left
    for c in range(3):
        for g in range(half // width):
            row = nodes_ref[c : c + 1, half + g * width : half + (g + 1) * width]
            spread_ref[c, g * width : (g + 1) * width, :] = jnp.broadcast_to(row, (width, width)).T
    best_ref[...] = jnp.full((count, width), penalty, jnp.float32)
    sublane = lax.broadcasted_iota(jnp.int32, (2 * FEAT, width), 0)
    chunk = 64
    unroll = 4

    def some_sources(i, carry):
        for u in range(unroll):
            base = (i * unroll + u) * SEND_ROWS
            sides = []
            for t in range(CAP // 2):
                tile = arrived_ref[pl.ds(base + t * 2 * FEAT, 2 * FEAT), :]
                for part in range(2):
                    kept = jnp.where((sublane >= FEAT) == (part == 1), tile, 0.0)
                    rows = stack_terms(*split3(kept)) + [jnp.zeros((entries, width), jnp.bfloat16)]
                    sides.append(jnp.concatenate(rows, axis=0))
            gaps = jnp.dot(left_ref[0:half, :], jnp.concatenate(sides, axis=1), preferred_element_type=jnp.float32)
            least = best_ref[0:half, :]
            for s in range(CAP):
                least = jnp.minimum(least, gaps[:, s * width : (s + 1) * width])
            best_ref[0:half, :] = least
            for j in range(half // chunk):
                x, y, z = [spread_ref[c, j * chunk : (j + 1) * chunk, :] for c in range(3)]
                here = slice(half + j * chunk, half + (j + 1) * chunk)
                least = best_ref[here, :]
                for s in range(CAP):
                    lx, ly, lz, off = [arrived_ref[pl.ds(base + s * FEAT + c, 1), :] for c in range(FEAT)]
                    least = jnp.minimum(least, (x * lx + y * ly) + (z * lz + off))
                best_ref[here, :] = least
        return carry

    lax.fori_loop(0, parts // unroll, some_sources, 0)
    finish(best_ref, nodes_ref, out_ref)


def finish(best_ref, nodes_ref, out_ref, most=None):
    width = best_ref.shape[1]
    for g in range(nodes_ref.shape[1] // width):
        here = slice(g * width, (g + 1) * width)
        least = jnp.min(best_ref[here, :].T, axis=0, keepdims=True)
        px, py, pz = [nodes_ref[c : c + 1, here] for c in range(3)]
        gap = least + (px * px + py * py + pz * pz)
        out_ref[:, here] = gap if most is None else jnp.minimum(most, gap)


def ghost_kernel(wanted_ref, reply_ref, nodes_ref, left_ref, out_ref, best_ref, *, blocks):
    entries = wanted_ref.shape[1]
    width = reply_ref.shape[1]
    holders = [wanted_ref[0, e] // blocks for e in range(entries)]
    slot = lax.broadcasted_iota(jnp.int32, (2 * FEAT, width), 0) // FEAT
    choice = lax.broadcasted_iota(jnp.int32, (entries, width), 0)
    sides = []
    for e in range(entries):
        order = 0
        for before in range(e):
            order = order + jnp.where(holders[before] == holders[e], 1, 0)
        tile = reply_ref[pl.ds(pl.multiple_of(holders[e] * REPLY_ROWS, REPLY_ROWS), REPLY_ROWS), :]
        kept = jnp.where(slot == order, tile, 0.0)
        rows = stack_terms(*split3(kept)) + [to_one(choice == e).astype(jnp.bfloat16)]
        sides.append(jnp.concatenate(rows, axis=0))
    gaps = jnp.dot(left_ref[...], jnp.concatenate(sides, axis=1), preferred_element_type=jnp.float32)
    least = gaps[:, 0:width]
    for e in range(1, entries):
        least = jnp.minimum(least, gaps[:, e * width : (e + 1) * width])
    best_ref[...] = least
    finish(best_ref, nodes_ref, out_ref, far_gap)


def exchange(rows, parts):
    per_part = rows.shape[0] // parts
    shaped = rows.reshape(parts, per_part, 1, rows.shape[1])
    moved = lax.all_to_all(shaped, AXES, split_axis=0, concat_axis=0, tiled=True)
    return moved.reshape(rows.shape)


def local(facets, owner, ghosts, ghost_count, nodes, cand):
    parts = lax.axis_size(AXES)
    blocks, _, width = facets.shape
    count = nodes.shape[1]
    entries = ghosts.shape[1]
    f32 = jnp.float32
    smem = pl.BlockSpec(memory_space=pltpu.SMEM)
    vmem = pl.BlockSpec(memory_space=pltpu.VMEM)
    params = pltpu.CompilerParams(vmem_limit_bytes=16 * 1024 * 1024)
    outgoing, table = pl.pallas_call(
        pack_kernel,
        out_shape=(
            jax.ShapeDtypeStruct((parts * SEND_ROWS, width), f32),
            jax.ShapeDtypeStruct((3 * blocks, FEAT * width), jnp.bfloat16),
        ),
        name="pack",
        compiler_params=params,
    )(jnp.transpose(facets, (1, 0, 2)), owner.T, ghosts)
    arrived = exchange(outgoing, parts)
    answer = pl.pallas_call(
        select_kernel, out_shape=jax.ShapeDtypeStruct((parts * REPLY_ROWS, width), f32), name="select", compiler_params=params
    )(arrived, table)
    reply = exchange(answer, parts)
    own_gap, left = pl.pallas_call(
        own_kernel,
        out_shape=(
            jax.ShapeDtypeStruct((1, count), f32),
            jax.ShapeDtypeStruct((count, 6 * 2 * FEAT + entries), jnp.bfloat16),
        ),
        in_specs=[smem, vmem, vmem, vmem],
        scratch_shapes=[pltpu.VMEM((3, count // 2, width), f32), pltpu.VMEM((count, width), f32)],
        name="own",
        compiler_params=params,
        cost_estimate=pl.CostEstimate(
            flops=7 * parts * CAP * width * count, bytes_accessed=parts * SEND_ROWS * width * 4, transcendentals=0
        ),
    )(ghost_count, arrived, nodes, cand)
    ghost_gap = pl.pallas_call(
        functools.partial(ghost_kernel, blocks=blocks),
        out_shape=jax.ShapeDtypeStruct((1, count), f32),
        in_specs=[smem, vmem, vmem, vmem],
        scratch_shapes=[pltpu.VMEM((count, width), f32)],
        name="ghost",
        compiler_params=params,
    )(ghosts, reply, nodes, left)
    return own_gap.reshape(count), ghost_gap.reshape(count)


def solution(mesh):
    return jax.shard_map(
        local,
        mesh=mesh,
        in_specs=(
            P(AXES, None, None),
            P(AXES, None),
            P(AXES, None),
            P(AXES),
            P(None, AXES),
            P(None, AXES),
        ),
        out_specs=(P(AXES), P(AXES)),
        check_vma=False,
    )
```

```python
import functools

import jax
import jax.numpy as jnp
from jax import lax
from jax.experimental import pallas as pl
from jax.experimental.pallas import tpu as pltpu
from jax.sharding import PartitionSpec as P

CAP = 4
GC = 2
FEAT = 4
OWN_ROWS = CAP * FEAT
SEND_ROWS = OWN_ROWS + 1
REPLY_ROWS = GC * FEAT
UNROLL = 8
CHUNK = 64
GHOST_CHUNKS = 3
AXES = ("gx", "gy")

far_gap = 10.0
penalty = 1e30


def split3(value):
    high = value.astype(jnp.bfloat16)
    rest = value - high.astype(jnp.float32)
    middle = rest.astype(jnp.bfloat16)
    low = (rest - middle.astype(jnp.float32)).astype(jnp.bfloat16)
    return high, middle, low


def to_one(flag):
    return jnp.where(flag, 1.0, 0.0)


def pack_kernel(facets_hbm, owner_hbm, ghosts_hbm, out_ref, feat_ref, facets_ref, owner_ref, ghosts_ref, sems):
    _, blocks, width = facets_ref.shape
    parts = out_ref.shape[0] // SEND_ROWS
    fetches = [
        pltpu.make_async_copy(source, target, sems.at[i])
        for i, (source, target) in enumerate(
            ((ghosts_hbm, ghosts_ref), (owner_hbm, owner_ref), (facets_hbm, facets_ref))
        )
    ]
    for fetch in fetches:
        fetch.start()
    fetches[0].wait()
    fetches[1].wait()
    owner_row = owner_ref[...]
    row_id = lax.broadcasted_iota(jnp.int32, (blocks, blocks), 0)
    col_id = lax.broadcasted_iota(jnp.int32, (blocks, blocks), 1)
    owner_col = jnp.sum(jnp.where(row_id == col_id, owner_row, 0), axis=1, keepdims=True)
    earlier = (owner_col == owner_row) & (row_id < col_id)
    rank = jnp.sum(jnp.where(earlier, 1, 0), axis=0, keepdims=True)
    part_id = lax.broadcasted_iota(jnp.int32, (parts, blocks), 0)
    mine = owner_row == part_id
    picks = [to_one(mine & (rank == s)) for s in range(CAP)]
    pick = jnp.concatenate(picks, axis=0).astype(jnp.bfloat16)
    wanted = ghosts_ref[...]
    entries = wanted.shape[1]
    part_of = lax.broadcasted_iota(jnp.int32, (parts, entries), 0)
    entry = lax.broadcasted_iota(jnp.int32, (parts, entries), 1)
    holder = wanted // blocks
    local_row = wanted - holder * blocks
    held = part_of == holder
    first = jnp.min(jnp.where(held, entry, entries), axis=1, keepdims=True)
    last = jnp.max(jnp.where(held, entry, -1), axis=1, keepdims=True)
    row_first = jnp.sum(jnp.where(held & (entry == first), local_row, 0), axis=1, keepdims=True)
    row_last = jnp.sum(jnp.where(held & (entry == last), local_row, 0), axis=1, keepdims=True)
    lane = lax.broadcasted_iota(jnp.int32, (parts, width), 1)
    request = jnp.where(lane == 0, row_first, jnp.where(lane == 1, row_last, 0))
    out_ref[pl.ds(OWN_ROWS, parts, stride=SEND_ROWS), :] = request.astype(jnp.float32)

    fetches[2].wait()
    ax, ay, az, bx, by, bz, cx, cy, cz, nx, ny, nz = [facets_ref[i] for i in range(12)]
    third = 1.0 / 3.0
    squares = lambda u, v, w: u * u + v * v + w * w
    spread = (squares(ax, bx, cx) + squares(ay, by, cy) + squares(az, bz, cz)) * third
    offset = spread - (nx * ax + ny * ay + nz * az)
    feats = [n - (2.0 * third) * (a + b + c) for n, a, b, c in ((nx, ax, bx, cx), (ny, ay, by, cy), (nz, az, bz, cz))]
    feats.append(offset)
    splits = [split3(f) for f in feats]
    table = jnp.concatenate(
        [jnp.concatenate([splits[c][i] for c in range(FEAT)], axis=1) for i in range(3)], axis=0
    )
    feat_ref[...] = table

    placed = jnp.dot(jnp.concatenate([pick] * 3, axis=1), table, preferred_element_type=jnp.float32)
    for s in range(CAP):
        absent = 1.0 - jnp.sum(picks[s], axis=1, keepdims=True)
        for c in range(FEAT):
            piece = placed[s * parts : (s + 1) * parts, c * width : (c + 1) * width]
            if c == FEAT - 1:
                piece = piece + penalty * absent
            out_ref[pl.ds(s * FEAT + c, parts, stride=SEND_ROWS), :] = piece


def select_kernel(arrived_ref, feat_ref, out_ref):
    parts = arrived_ref.shape[0] // SEND_ROWS
    width = arrived_ref.shape[1]
    blocks = feat_ref.shape[0] // 3
    request = arrived_ref[pl.ds(OWN_ROWS, parts, stride=SEND_ROWS), :].astype(jnp.int32)
    block_id = lax.broadcasted_iota(jnp.int32, (parts, blocks), 1)
    pick = jnp.concatenate([to_one(request[:, s : s + 1] == block_id) for s in range(GC)], axis=0)
    pick = pick.astype(jnp.bfloat16)
    rows = jnp.dot(jnp.concatenate([pick] * 3, axis=1), feat_ref[...], preferred_element_type=jnp.float32)
    for s in range(GC):
        for c in range(FEAT):
            out_ref[pl.ds(s * FEAT + c, parts, stride=REPLY_ROWS), :] = rows[
                s * parts : (s + 1) * parts, c * width : (c + 1) * width
            ]


def stack_terms(high, middle, low):
    return [high, high, high, middle, middle, low]


def point_terms(points):
    four = jnp.concatenate([points, jnp.ones_like(points[0:1])], axis=0)
    high, middle, low = [t.astype(jnp.float32) for t in split3(jnp.concatenate([four, four], axis=0))]
    return [high, middle, low, high, middle, high]


def prep_kernel(limit_ref, wanted_ref, nodes_ref, cand_ref, left_ref, spread_ref, shade_ref, place_ref, *, blocks):
    count = nodes_ref.shape[1]
    _, half, width = spread_ref.shape
    entries = wanted_ref.shape[1]
    holder = wanted_ref[...] // blocks
    row_id = lax.broadcasted_iota(jnp.int32, (entries, entries), 0)
    col_id = lax.broadcasted_iota(jnp.int32, (entries, entries), 1)
    holder_col = jnp.sum(jnp.where(row_id == col_id, holder, 0), axis=1, keepdims=True)
    earlier = (holder_col == holder) & (row_id < col_id)
    order = jnp.sum(jnp.where(earlier, 1, 0), axis=0, keepdims=True)
    place_ref[0:1, :] = holder * REPLY_ROWS
    place_ref[1:2, :] = order
    entry = lax.broadcasted_iota(jnp.int32, (entries, count), 0)
    chosen = entry == cand_ref[0:1, :]
    for k in range(1, cand_ref.shape[0]):
        chosen = chosen | (entry == cand_ref[k : k + 1, :])
    mask = jnp.where(chosen & (entry < limit_ref[0]), 0.0, penalty)
    left_ref[...] = jnp.concatenate(point_terms(nodes_ref[...]) + [mask], axis=0).T.astype(jnp.bfloat16)
    shade_ref[...] = mask[:, half:].T
    for c in range(3):
        for g in range(half // width):
            row = nodes_ref[c : c + 1, half + g * width : half + (g + 1) * width]
            spread_ref[c, g * width : (g + 1) * width, :] = jnp.broadcast_to(row, (width, width)).T


def own_kernel(arrived_ref, left_ref, spread_ref, out_ref, best_ref):
    parts = arrived_ref.shape[0] // SEND_ROWS
    width = arrived_ref.shape[1]
    count = left_ref.shape[0]
    half = count // 2
    entries = left_ref.shape[1] - 6 * 2 * FEAT
    best_ref[...] = jnp.full((count, width), penalty, jnp.float32)
    sublane = lax.broadcasted_iota(jnp.int32, (2 * FEAT, width), 0)
    chunk = CHUNK
    unroll = UNROLL

    def some_sources(i, carry):
        for u in range(unroll):
            base = (i * unroll + u) * SEND_ROWS
            sides = []
            for t in range(CAP // 2):
                tile = arrived_ref[pl.ds(base + t * 2 * FEAT, 2 * FEAT), :]
                for part in range(2):
                    kept = jnp.where((sublane >= FEAT) == (part == 1), tile, 0.0)
                    rows = stack_terms(*split3(kept)) + [jnp.zeros((entries, width), jnp.bfloat16)]
                    sides.append(jnp.concatenate(rows, axis=0))
            gaps = jnp.dot(left_ref[0:half, :], jnp.concatenate(sides, axis=1), preferred_element_type=jnp.float32)
            least = best_ref[0:half, :]
            for s in range(CAP):
                least = jnp.minimum(least, gaps[:, s * width : (s + 1) * width])
            best_ref[0:half, :] = least
            for j in range(half // chunk):
                x, y, z = [spread_ref[c, j * chunk : (j + 1) * chunk, :] for c in range(3)]
                here = slice(half + j * chunk, half + (j + 1) * chunk)
                least = best_ref[here, :]
                for s in range(CAP):
                    lx, ly, lz, off = [arrived_ref[pl.ds(base + s * FEAT + c, 1), :] for c in range(FEAT)]
                    least = jnp.minimum(least, (x * lx + y * ly) + (z * lz + off))
                best_ref[here, :] = least
        return carry

    lax.fori_loop(0, parts // unroll, some_sources, 0)
    for g in range(count // width):
        here = slice(g * width, (g + 1) * width)
        out_ref[:, here] = jnp.min(best_ref[here, :].T, axis=0, keepdims=True)


def ghost_kernel(
    place_ref, reply_ref, nodes_ref, left_ref, spread_ref, shade_ref, own_ref, own_out_ref, out_ref, best_ref
):
    entries = place_ref.shape[1]
    count = nodes_ref.shape[1]
    width = reply_ref.shape[1]
    half = spread_ref.shape[1]
    first = count - GHOST_CHUNKS * CHUNK
    place = place_ref[...]
    slot = lax.broadcasted_iota(jnp.int32, (2 * FEAT, width), 0) // FEAT
    choice = lax.broadcasted_iota(jnp.int32, (entries, width), 0)
    sides = []
    starts = []
    for e in range(entries):
        start, order = place[0, e], place[1, e]
        starts.append(start + order * FEAT)
        tile = reply_ref[pl.ds(pl.multiple_of(start, REPLY_ROWS), REPLY_ROWS), :]
        kept = jnp.where(slot == order, tile, 0.0)
        rows = stack_terms(*split3(kept)) + [to_one(choice == e).astype(jnp.bfloat16)]
        sides.append(jnp.concatenate(rows, axis=0))
    gaps = jnp.dot(left_ref[0:first, :], jnp.concatenate(sides, axis=1), preferred_element_type=jnp.float32)
    least = gaps[:, 0:width]
    for e in range(1, entries):
        least = jnp.minimum(least, gaps[:, e * width : (e + 1) * width])
    best_ref[0:first, :] = least
    for j in range(first, count, CHUNK):
        here = slice(j - (count - half), j - (count - half) + CHUNK)
        x, y, z = [spread_ref[c, here, :] for c in range(3)]
        least = jnp.full((CHUNK, width), penalty, jnp.float32)
        for e in range(entries):
            lx, ly, lz, off = [reply_ref[pl.ds(starts[e] + c, 1), :] for c in range(FEAT)]
            shade = jnp.broadcast_to(shade_ref[here, e : e + 1], (CHUNK, width))
            least = jnp.minimum(least, ((x * lx + y * ly) + (z * lz + off)) + shade)
        best_ref[j : j + CHUNK, :] = least
    px, py, pz = [nodes_ref[c : c + 1, :] for c in range(3)]
    square = px * px + py * py + pz * pz
    own_out_ref[...] = own_ref[...] + square
    for g in range(count // width):
        here = slice(g * width, (g + 1) * width)
        least = jnp.min(best_ref[here, :].T, axis=0, keepdims=True)
        out_ref[:, here] = jnp.minimum(far_gap, least + square[:, here])


def exchange(rows, parts):
    per_part = rows.shape[0] // parts
    shaped = rows.reshape(parts, per_part, 1, rows.shape[1])
    moved = lax.all_to_all(shaped, AXES, split_axis=0, concat_axis=0, tiled=True)
    return moved.reshape(rows.shape)


def local(facets, owner, ghosts, ghost_count, nodes, cand):
    parts = lax.axis_size(AXES)
    blocks, _, width = facets.shape
    count = nodes.shape[1]
    entries = ghosts.shape[1]
    f32 = jnp.float32
    smem = pl.BlockSpec(memory_space=pltpu.SMEM)
    vmem = pl.BlockSpec(memory_space=pltpu.VMEM)
    params = pltpu.CompilerParams(vmem_limit_bytes=16 * 1024 * 1024)
    hbm = pl.BlockSpec(memory_space=pltpu.HBM)
    outgoing, table = pl.pallas_call(
        pack_kernel,
        out_shape=(
            jax.ShapeDtypeStruct((parts * SEND_ROWS, width), f32),
            jax.ShapeDtypeStruct((3 * blocks, FEAT * width), jnp.bfloat16),
        ),
        in_specs=[hbm] * 3,
        out_specs=(vmem, vmem),
        scratch_shapes=[
            pltpu.VMEM((12, blocks, width), f32),
            pltpu.VMEM((1, blocks), jnp.int32),
            pltpu.VMEM((1, entries), jnp.int32),
            pltpu.SemaphoreType.DMA((3,)),
        ],
        name="pack",
        compiler_params=params,
    )(*[pltpu.with_memory_space_constraint(v, pltpu.HBM) for v in (jnp.transpose(facets, (1, 0, 2)), owner.T, ghosts)])
    arrived = exchange(outgoing, parts)
    left, spread, shade, place = pl.pallas_call(
        functools.partial(prep_kernel, blocks=blocks),
        out_shape=(
            jax.ShapeDtypeStruct((count, 6 * 2 * FEAT + entries), jnp.bfloat16),
            jax.ShapeDtypeStruct((3, count // 2, width), f32),
            jax.ShapeDtypeStruct((count // 2, entries), f32),
            jax.ShapeDtypeStruct((2, entries), jnp.int32),
        ),
        in_specs=[smem, vmem, vmem, vmem],
        out_specs=(vmem, vmem, vmem, vmem),
        name="prep",
        compiler_params=params,
    )(ghost_count, ghosts, nodes, cand)
    answer = pl.pallas_call(
        select_kernel,
        out_shape=jax.ShapeDtypeStruct((parts * REPLY_ROWS, width), f32),
        in_specs=[vmem, vmem],
        out_specs=vmem,
        name="select",
        compiler_params=params,
    )(arrived, table)
    reply = exchange(answer, parts)
    own_least = pl.pallas_call(
        own_kernel,
        out_shape=jax.ShapeDtypeStruct((1, count), f32),
        in_specs=[vmem] * 3,
        out_specs=vmem,
        scratch_shapes=[pltpu.VMEM((count, width), f32)],
        name="own",
        compiler_params=params,
        cost_estimate=pl.CostEstimate(
            flops=7 * parts * CAP * width * count, bytes_accessed=parts * SEND_ROWS * width * 4, transcendentals=0
        ),
    )(arrived, left, spread)
    own_gap, ghost_gap = pl.pallas_call(
        ghost_kernel,
        out_shape=[jax.ShapeDtypeStruct((1, count), f32)] * 2,
        in_specs=[vmem] * 7,
        out_specs=[vmem, vmem],
        scratch_shapes=[pltpu.VMEM((count, width), f32)],
        name="ghost",
        compiler_params=params,
    )(place, reply, nodes, left, spread, shade, own_least)
    return own_gap.reshape(count), ghost_gap.reshape(count)


def solution(mesh):
    return jax.shard_map(
        local,
        mesh=mesh,
        in_specs=(
            P(AXES, None, None),
            P(AXES, None),
            P(AXES, None),
            P(AXES),
            P(None, AXES),
            P(None, AXES),
        ),
        out_specs=(P(AXES), P(AXES)),
        check_vma=False,
    )
```

```python
import functools

import jax
import jax.numpy as jnp
from jax import lax
from jax.experimental import pallas as pl
from jax.experimental.pallas import tpu as pltpu
from jax.sharding import PartitionSpec as P

CAP = 4
GC = 2
FEAT = 4
OWN_ROWS = CAP * FEAT
SEND_ROWS = OWN_ROWS + 1
REPLY_ROWS = GC * FEAT
UNROLL = 8
CHUNK = 64
GHOST_CHUNKS = 2
GHOST_GROUP = 8
AXES = ("gx", "gy")

far_gap = 10.0
penalty = 1e30


def split3(value):
    high = value.astype(jnp.bfloat16)
    rest = value - high.astype(jnp.float32)
    middle = rest.astype(jnp.bfloat16)
    low = (rest - middle.astype(jnp.float32)).astype(jnp.bfloat16)
    return high, middle, low


def to_one(flag):
    return jnp.where(flag, 1.0, 0.0)


def pack_kernel(facets_hbm, owner_hbm, ghosts_hbm, out_ref, table_ref, facets_ref, owner_ref, ghosts_ref, sems):
    _, blocks, width = facets_ref.shape
    parts = out_ref.shape[0] // SEND_ROWS
    fetches = [
        pltpu.make_async_copy(source, target, sems.at[i])
        for i, (source, target) in enumerate(
            ((ghosts_hbm, ghosts_ref), (owner_hbm, owner_ref), (facets_hbm, facets_ref))
        )
    ]
    for fetch in fetches:
        fetch.start()
    fetches[0].wait()
    fetches[1].wait()
    owner_row = owner_ref[...]
    row_id = lax.broadcasted_iota(jnp.int32, (blocks, blocks), 0)
    col_id = lax.broadcasted_iota(jnp.int32, (blocks, blocks), 1)
    owner_col = jnp.sum(jnp.where(row_id == col_id, owner_row, 0), axis=1, keepdims=True)
    earlier = (owner_col == owner_row) & (row_id < col_id)
    rank = jnp.sum(jnp.where(earlier, 1, 0), axis=0, keepdims=True)
    places = owner_row * SEND_ROWS + rank * FEAT
    starts = [places[0, b] for b in range(blocks)]
    out_ref[...] = jnp.zeros(out_ref.shape, jnp.float32)
    for slot in range(CAP):
        out_ref[pl.ds(slot * FEAT + FEAT - 1, parts, stride=SEND_ROWS), :] = jnp.full((parts, width), penalty, jnp.float32)

    wanted = ghosts_ref[...]
    entries = wanted.shape[1]
    part_of = lax.broadcasted_iota(jnp.int32, (parts, entries), 0)
    entry = lax.broadcasted_iota(jnp.int32, (parts, entries), 1)
    holder = wanted // blocks
    local_row = wanted - holder * blocks
    held = part_of == holder
    first = jnp.min(jnp.where(held, entry, entries), axis=1, keepdims=True)
    last = jnp.max(jnp.where(held, entry, -1), axis=1, keepdims=True)
    row_first = jnp.sum(jnp.where(held & (entry == first), local_row, 0), axis=1, keepdims=True)
    row_last = jnp.sum(jnp.where(held & (entry == last), local_row, 0), axis=1, keepdims=True)
    lane = lax.broadcasted_iota(jnp.int32, (parts, width), 1)
    request = jnp.where(lane == 0, row_first, jnp.where(lane == 1, row_last, 0))
    out_ref[pl.ds(OWN_ROWS, parts, stride=SEND_ROWS), :] = request.astype(jnp.float32)

    fetches[2].wait()
    ax, ay, az, bx, by, bz, cx, cy, cz, nx, ny, nz = [facets_ref[i] for i in range(12)]
    third = 1.0 / 3.0
    squares = lambda u, v, w: u * u + v * v + w * w
    spread = (squares(ax, bx, cx) + squares(ay, by, cy) + squares(az, bz, cz)) * third
    offset = spread - (nx * ax + ny * ay + nz * az)
    feats = [n - (2.0 * third) * (a + b + c) for n, a, b, c in ((nx, ax, bx, cx), (ny, ay, by, cy), (nz, az, bz, cz))]
    feats.append(offset)
    for c in range(FEAT):
        table_ref[pl.ds(c, blocks, stride=FEAT), :] = feats[c]
    for b in range(blocks):
        out_ref[pl.ds(starts[b], FEAT), :] = table_ref[b * FEAT : (b + 1) * FEAT, :]


def select_kernel(arrived_ref, table_ref, out_ref):
    parts = arrived_ref.shape[0] // SEND_ROWS
    request = arrived_ref[pl.ds(OWN_ROWS, parts, stride=SEND_ROWS), :].astype(jnp.int32) * FEAT
    for d in range(parts):
        for s in range(GC):
            row = d * REPLY_ROWS + s * FEAT
            out_ref[row : row + FEAT, :] = table_ref[pl.ds(pl.multiple_of(request[d, s], FEAT), FEAT), :]


def stack_terms(high, middle, low):
    return [high, high, high, middle, middle, low]


def point_terms(points):
    four = jnp.concatenate([points, jnp.ones_like(points[0:1])], axis=0)
    high, middle, low = [t.astype(jnp.float32) for t in split3(jnp.concatenate([four, four], axis=0))]
    return [high, middle, low, high, middle, high]


def prep_kernel(limit_ref, wanted_ref, nodes_ref, cand_ref, left_ref, spread_ref, shade_ref, place_ref, *, blocks):
    count = nodes_ref.shape[1]
    _, half, width = spread_ref.shape
    entries = wanted_ref.shape[1]
    holder = wanted_ref[...] // blocks
    row_id = lax.broadcasted_iota(jnp.int32, (entries, entries), 0)
    col_id = lax.broadcasted_iota(jnp.int32, (entries, entries), 1)
    holder_col = jnp.sum(jnp.where(row_id == col_id, holder, 0), axis=1, keepdims=True)
    earlier = (holder_col == holder) & (row_id < col_id)
    order = jnp.sum(jnp.where(earlier, 1, 0), axis=0, keepdims=True)
    place_ref[0:1, :] = holder * REPLY_ROWS
    place_ref[1:2, :] = order
    entry = lax.broadcasted_iota(jnp.int32, (entries, count), 0)
    chosen = entry == cand_ref[0:1, :]
    for k in range(1, cand_ref.shape[0]):
        chosen = chosen | (entry == cand_ref[k : k + 1, :])
    mask = jnp.where(chosen & (entry < limit_ref[0]), 0.0, penalty)
    left_ref[...] = jnp.concatenate(point_terms(nodes_ref[...]) + [mask], axis=0).T.astype(jnp.bfloat16)
    shade_ref[...] = mask[:, half:].T
    for c in range(3):
        for g in range(half // width):
            row = nodes_ref[c : c + 1, half + g * width : half + (g + 1) * width]
            spread_ref[c, g * width : (g + 1) * width, :] = jnp.broadcast_to(row, (width, width)).T


def own_kernel(arrived_ref, left_ref, spread_ref, out_ref, best_ref):
    parts = arrived_ref.shape[0] // SEND_ROWS
    width = arrived_ref.shape[1]
    count = left_ref.shape[0]
    half = count // 2
    entries = left_ref.shape[1] - 6 * 2 * FEAT
    best_ref[...] = jnp.full((count, width), penalty, jnp.float32)
    sublane = lax.broadcasted_iota(jnp.int32, (2 * FEAT, width), 0)
    chunk = CHUNK
    unroll = UNROLL

    def some_sources(i, carry):
        for u in range(unroll):
            base = (i * unroll + u) * SEND_ROWS
            sides = []
            for t in range(CAP // 2):
                tile = arrived_ref[pl.ds(base + t * 2 * FEAT, 2 * FEAT), :]
                for part in range(2):
                    kept = jnp.where((sublane >= FEAT) == (part == 1), tile, 0.0)
                    rows = stack_terms(*split3(kept)) + [jnp.zeros((entries, width), jnp.bfloat16)]
                    sides.append(jnp.concatenate(rows, axis=0))
            gaps = jnp.dot(left_ref[0:half, :], jnp.concatenate(sides, axis=1), preferred_element_type=jnp.float32)
            least = best_ref[0:half, :]
            for s in range(CAP):
                least = jnp.minimum(least, gaps[:, s * width : (s + 1) * width])
            best_ref[0:half, :] = least
            for j in range(half // chunk):
                x, y, z = [spread_ref[c, j * chunk : (j + 1) * chunk, :] for c in range(3)]
                here = slice(half + j * chunk, half + (j + 1) * chunk)
                least = best_ref[here, :]
                for s in range(CAP):
                    lx, ly, lz, off = [arrived_ref[pl.ds(base + s * FEAT + c, 1), :] for c in range(FEAT)]
                    least = jnp.minimum(least, (x * lx + y * ly) + (z * lz + off))
                best_ref[here, :] = least
        return carry

    lax.fori_loop(0, parts // unroll, some_sources, 0)
    for g in range(count // width):
        here = slice(g * width, (g + 1) * width)
        out_ref[:, here] = jnp.min(best_ref[here, :].T, axis=0, keepdims=True)


def ghost_kernel(
    limit_ref, place_ref, reply_ref, nodes_ref, left_ref, spread_ref, shade_ref, own_ref, own_out_ref, out_ref, best_ref
):
    entries = place_ref.shape[1]
    count = nodes_ref.shape[1]
    width = reply_ref.shape[1]
    half = spread_ref.shape[1]
    first = count - GHOST_CHUNKS * CHUNK
    place = place_ref[...]
    slot = lax.broadcasted_iota(jnp.int32, (2 * FEAT, width), 0) // FEAT
    choice = lax.broadcasted_iota(jnp.int32, (entries, width), 0)
    best_ref[...] = jnp.full((count, width), penalty, jnp.float32)
    def some_entries(members):
        sides = []
        starts = []
        for e in members:
            start, order = place[0, e], place[1, e]
            starts.append(start + order * FEAT)
            tile = reply_ref[pl.ds(pl.multiple_of(start, REPLY_ROWS), REPLY_ROWS), :]
            kept = jnp.where(slot == order, tile, 0.0)
            rows = stack_terms(*split3(kept)) + [to_one(choice == e).astype(jnp.bfloat16)]
            sides.append(jnp.concatenate(rows, axis=0))
        gaps = jnp.dot(left_ref[0:first, :], jnp.concatenate(sides, axis=1), preferred_element_type=jnp.float32)
        least = best_ref[0:first, :]
        for i in range(len(sides)):
            least = jnp.minimum(least, gaps[:, i * width : (i + 1) * width])
        best_ref[0:first, :] = least
        for j in range(first, count, CHUNK):
            here = slice(j - (count - half), j - (count - half) + CHUNK)
            x, y, z = [spread_ref[c, here, :] for c in range(3)]
            least = best_ref[j : j + CHUNK, :]
            for e, start in zip(members, starts):
                lx, ly, lz, off = [reply_ref[pl.ds(start + c, 1), :] for c in range(FEAT)]
                shade = jnp.broadcast_to(shade_ref[here, e : e + 1], (CHUNK, width))
                least = jnp.minimum(least, ((x * lx + y * ly) + (z * lz + off)) + shade)
            best_ref[j : j + CHUNK, :] = least

    for group in range(0, entries, GHOST_GROUP):
        members = range(group, min(group + GHOST_GROUP, entries))
        if group == 0:
            some_entries(members)
        else:
            pl.when(limit_ref[0] > group)(functools.partial(some_entries, members))
    px, py, pz = [nodes_ref[c : c + 1, :] for c in range(3)]
    square = px * px + py * py + pz * pz
    own_out_ref[...] = own_ref[...] + square
    for g in range(count // width):
        here = slice(g * width, (g + 1) * width)
        least = jnp.min(best_ref[here, :].T, axis=0, keepdims=True)
        out_ref[:, here] = jnp.minimum(far_gap, least + square[:, here])


def exchange(rows, parts):
    per_part = rows.shape[0] // parts
    shaped = rows.reshape(parts, per_part, 1, rows.shape[1])
    moved = lax.all_to_all(shaped, AXES, split_axis=0, concat_axis=0, tiled=True)
    return moved.reshape(rows.shape)


def local(facets, owner, ghosts, ghost_count, nodes, cand):
    parts = lax.axis_size(AXES)
    blocks, _, width = facets.shape
    count = nodes.shape[1]
    entries = ghosts.shape[1]
    f32 = jnp.float32
    smem = pl.BlockSpec(memory_space=pltpu.SMEM)
    vmem = pl.BlockSpec(memory_space=pltpu.VMEM)
    params = pltpu.CompilerParams(vmem_limit_bytes=16 * 1024 * 1024)
    hbm = pl.BlockSpec(memory_space=pltpu.HBM)
    outgoing, table = pl.pallas_call(
        pack_kernel,
        out_shape=(
            jax.ShapeDtypeStruct((parts * SEND_ROWS, width), f32),
            jax.ShapeDtypeStruct((blocks * FEAT, width), f32),
        ),
        in_specs=[hbm] * 3,
        out_specs=(vmem, vmem),
        scratch_shapes=[
            pltpu.VMEM((12, blocks, width), f32),
            pltpu.VMEM((1, blocks), jnp.int32),
            pltpu.VMEM((1, entries), jnp.int32),
            pltpu.SemaphoreType.DMA((3,)),
        ],
        name="pack",
        compiler_params=params,
    )(*[pltpu.with_memory_space_constraint(v, pltpu.HBM) for v in (jnp.transpose(facets, (1, 0, 2)), owner.T, ghosts)])
    arrived = exchange(outgoing, parts)
    left, spread, shade, place = pl.pallas_call(
        functools.partial(prep_kernel, blocks=blocks),
        out_shape=(
            jax.ShapeDtypeStruct((count, 6 * 2 * FEAT + entries), jnp.bfloat16),
            jax.ShapeDtypeStruct((3, count // 2, width), f32),
            jax.ShapeDtypeStruct((count // 2, entries), f32),
            jax.ShapeDtypeStruct((2, entries), jnp.int32),
        ),
        in_specs=[smem, vmem, vmem, vmem],
        out_specs=(vmem, vmem, vmem, vmem),
        name="prep",
        compiler_params=params,
    )(ghost_count, ghosts, nodes, cand)
    answer = pl.pallas_call(
        select_kernel,
        out_shape=jax.ShapeDtypeStruct((parts * REPLY_ROWS, width), f32),
        in_specs=[vmem, vmem],
        out_specs=vmem,
        name="select",
        compiler_params=params,
    )(arrived, table)
    reply = exchange(answer, parts)
    own_least = pl.pallas_call(
        own_kernel,
        out_shape=jax.ShapeDtypeStruct((1, count), f32),
        in_specs=[vmem] * 3,
        out_specs=vmem,
        scratch_shapes=[pltpu.VMEM((count, width), f32)],
        name="own",
        compiler_params=params,
        cost_estimate=pl.CostEstimate(
            flops=7 * parts * CAP * width * count, bytes_accessed=parts * SEND_ROWS * width * 4, transcendentals=0
        ),
    )(arrived, left, spread)
    own_gap, ghost_gap = pl.pallas_call(
        ghost_kernel,
        out_shape=[jax.ShapeDtypeStruct((1, count), f32)] * 2,
        in_specs=[smem] + [vmem] * 7,
        out_specs=[vmem, vmem],
        scratch_shapes=[pltpu.VMEM((count, width), f32)],
        name="ghost",
        compiler_params=params,
    )(ghost_count, place, reply, nodes, left, spread, shade, own_least)
    return own_gap.reshape(count), ghost_gap.reshape(count)


def solution(mesh):
    return jax.shard_map(
        local,
        mesh=mesh,
        in_specs=(
            P(AXES, None, None),
            P(AXES, None),
            P(AXES, None),
            P(AXES),
            P(None, AXES),
            P(None, AXES),
        ),
        out_specs=(P(AXES), P(AXES)),
        check_vma=False,
    )
```

```python
import functools

import jax
import jax.numpy as jnp
from jax import lax
from jax.experimental import pallas as pl
from jax.experimental.pallas import tpu as pltpu
from jax.sharding import PartitionSpec as P

CAP = 4
GC = 2
FEAT = 4
OWN_ROWS = CAP * FEAT
SEND_ROWS = OWN_ROWS + 1
REPLY_ROWS = GC * FEAT
UNROLL = 8
CHUNK = 64
GHOST_CHUNKS = 2
SPREAD = 128
GHOST_LEVELS = (4, 8, 1 << 30)
AXES = ("gx", "gy")

far_gap = 10.0
penalty = 1e30


def split3(value):
    high = value.astype(jnp.bfloat16)
    rest = value - high.astype(jnp.float32)
    middle = rest.astype(jnp.bfloat16)
    low = (rest - middle.astype(jnp.float32)).astype(jnp.bfloat16)
    return high, middle, low


def to_one(flag):
    return jnp.where(flag, 1.0, 0.0)


def pack_kernel(facets_hbm, owner_hbm, ghosts_hbm, out_ref, table_ref, facets_ref, owner_ref, ghosts_ref, sems):
    _, blocks, width = facets_ref.shape
    parts = out_ref.shape[0] // SEND_ROWS
    fetches = [
        pltpu.make_async_copy(source, target, sems.at[i])
        for i, (source, target) in enumerate(
            ((ghosts_hbm, ghosts_ref), (owner_hbm, owner_ref), (facets_hbm, facets_ref))
        )
    ]
    for fetch in fetches:
        fetch.start()
    fetches[0].wait()
    fetches[1].wait()
    owner_row = owner_ref[...]
    row_id = lax.broadcasted_iota(jnp.int32, (blocks, blocks), 0)
    col_id = lax.broadcasted_iota(jnp.int32, (blocks, blocks), 1)
    owner_col = jnp.sum(jnp.where(row_id == col_id, owner_row, 0), axis=1, keepdims=True)
    earlier = (owner_col == owner_row) & (row_id < col_id)
    rank = jnp.sum(jnp.where(earlier, 1, 0), axis=0, keepdims=True)
    places = owner_row * SEND_ROWS + rank * FEAT
    starts = [places[0, b] for b in range(blocks)]
    out_ref[...] = jnp.zeros(out_ref.shape, jnp.float32)
    for slot in range(CAP):
        out_ref[pl.ds(slot * FEAT + FEAT - 1, parts, stride=SEND_ROWS), :] = jnp.full((parts, width), penalty, jnp.float32)

    wanted = ghosts_ref[...]
    entries = wanted.shape[1]
    part_of = lax.broadcasted_iota(jnp.int32, (parts, entries), 0)
    entry = lax.broadcasted_iota(jnp.int32, (parts, entries), 1)
    holder = wanted // blocks
    local_row = wanted - holder * blocks
    held = part_of == holder
    first = jnp.min(jnp.where(held, entry, entries), axis=1, keepdims=True)
    last = jnp.max(jnp.where(held, entry, -1), axis=1, keepdims=True)
    row_first = jnp.sum(jnp.where(held & (entry == first), local_row, 0), axis=1, keepdims=True)
    row_last = jnp.sum(jnp.where(held & (entry == last), local_row, 0), axis=1, keepdims=True)
    lane = lax.broadcasted_iota(jnp.int32, (parts, width), 1)
    request = jnp.where(lane == 0, row_first, jnp.where(lane == 1, row_last, 0))
    out_ref[pl.ds(OWN_ROWS, parts, stride=SEND_ROWS), :] = request.astype(jnp.float32)

    fetches[2].wait()
    ax, ay, az, bx, by, bz, cx, cy, cz, nx, ny, nz = [facets_ref[i] for i in range(12)]
    third = 1.0 / 3.0
    squares = lambda u, v, w: u * u + v * v + w * w
    spread = (squares(ax, bx, cx) + squares(ay, by, cy) + squares(az, bz, cz)) * third
    offset = spread - (nx * ax + ny * ay + nz * az)
    feats = [n - (2.0 * third) * (a + b + c) for n, a, b, c in ((nx, ax, bx, cx), (ny, ay, by, cy), (nz, az, bz, cz))]
    feats.append(offset)
    for c in range(FEAT):
        table_ref[pl.ds(c, blocks, stride=FEAT), :] = feats[c]
    for b in range(blocks):
        out_ref[pl.ds(starts[b], FEAT), :] = table_ref[b * FEAT : (b + 1) * FEAT, :]


def select_kernel(arrived_ref, table_ref, out_ref):
    parts = arrived_ref.shape[0] // SEND_ROWS
    request = arrived_ref[pl.ds(OWN_ROWS, parts, stride=SEND_ROWS), :].astype(jnp.int32) * FEAT
    for d in range(parts):
        for s in range(GC):
            row = d * REPLY_ROWS + s * FEAT
            out_ref[row : row + FEAT, :] = table_ref[pl.ds(pl.multiple_of(request[d, s], FEAT), FEAT), :]


def stack_terms(high, middle, low):
    return [high, high, high, middle, middle, low]


def point_terms(points):
    four = jnp.concatenate([points, jnp.ones_like(points[0:1])], axis=0)
    high, middle, low = [t.astype(jnp.float32) for t in split3(jnp.concatenate([four, four], axis=0))]
    return [high, middle, low, high, middle, high]


def prep_kernel(limit_ref, wanted_ref, nodes_ref, cand_ref, left_ref, spread_ref, shade_ref, place_ref, *, blocks):
    count = nodes_ref.shape[1]
    _, spread_count, width = spread_ref.shape
    start = count - spread_count
    entries = wanted_ref.shape[1]
    holder = wanted_ref[...] // blocks
    row_id = lax.broadcasted_iota(jnp.int32, (entries, entries), 0)
    col_id = lax.broadcasted_iota(jnp.int32, (entries, entries), 1)
    holder_col = jnp.sum(jnp.where(row_id == col_id, holder, 0), axis=1, keepdims=True)
    earlier = (holder_col == holder) & (row_id < col_id)
    order = jnp.sum(jnp.where(earlier, 1, 0), axis=0, keepdims=True)
    place_ref[0:1, :] = holder * REPLY_ROWS
    place_ref[1:2, :] = order
    entry = lax.broadcasted_iota(jnp.int32, (entries, count), 0)
    chosen = entry == cand_ref[0:1, :]
    for k in range(1, cand_ref.shape[0]):
        chosen = chosen | (entry == cand_ref[k : k + 1, :])
    mask = jnp.where(chosen & (entry < limit_ref[0]), 0.0, penalty)
    left_ref[...] = jnp.concatenate(point_terms(nodes_ref[...]) + [mask], axis=0).T.astype(jnp.bfloat16)
    shade_ref[...] = mask[:, start:].T
    for c in range(3):
        for g in range(spread_count // width):
            row = nodes_ref[c : c + 1, start + g * width : start + (g + 1) * width]
            spread_ref[c, g * width : (g + 1) * width, :] = jnp.broadcast_to(row, (width, width)).T


def own_kernel(arrived_ref, left_ref, spread_ref, out_ref, best_ref):
    parts = arrived_ref.shape[0] // SEND_ROWS
    width = arrived_ref.shape[1]
    count = left_ref.shape[0]
    first = count - spread_ref.shape[1]
    entries = left_ref.shape[1] - 6 * 2 * FEAT
    best_ref[...] = jnp.full((count, width), penalty, jnp.float32)
    sublane = lax.broadcasted_iota(jnp.int32, (2 * FEAT, width), 0)
    chunk = CHUNK
    unroll = UNROLL

    def some_sources(i, carry):
        for u in range(unroll):
            base = (i * unroll + u) * SEND_ROWS
            sides = []
            for t in range(CAP // 2):
                tile = arrived_ref[pl.ds(base + t * 2 * FEAT, 2 * FEAT), :]
                for part in range(2):
                    kept = jnp.where((sublane >= FEAT) == (part == 1), tile, 0.0)
                    rows = stack_terms(*split3(kept)) + [jnp.zeros((entries, width), jnp.bfloat16)]
                    sides.append(jnp.concatenate(rows, axis=0))
            gaps = jnp.dot(left_ref[0:first, :], jnp.concatenate(sides, axis=1), preferred_element_type=jnp.float32)
            least = best_ref[0:first, :]
            for s in range(CAP):
                least = jnp.minimum(least, gaps[:, s * width : (s + 1) * width])
            best_ref[0:first, :] = least
            for j in range((count - first) // chunk):
                x, y, z = [spread_ref[c, j * chunk : (j + 1) * chunk, :] for c in range(3)]
                here = slice(first + j * chunk, first + (j + 1) * chunk)
                least = best_ref[here, :]
                for s in range(CAP):
                    lx, ly, lz, off = [arrived_ref[pl.ds(base + s * FEAT + c, 1), :] for c in range(FEAT)]
                    least = jnp.minimum(least, (x * lx + y * ly) + (z * lz + off))
                best_ref[here, :] = least
        return carry

    lax.fori_loop(0, parts // unroll, some_sources, 0)
    for g in range(count // width):
        here = slice(g * width, (g + 1) * width)
        out_ref[:, here] = jnp.min(best_ref[here, :].T, axis=0, keepdims=True)


def ghost_kernel(
    limit_ref, place_ref, reply_ref, nodes_ref, left_ref, spread_ref, shade_ref, own_ref, own_out_ref, out_ref, best_ref
):
    entries = place_ref.shape[1]
    count = nodes_ref.shape[1]
    width = reply_ref.shape[1]
    spread_start = count - spread_ref.shape[1]
    first = count - GHOST_CHUNKS * CHUNK
    place = place_ref[...]
    slot = lax.broadcasted_iota(jnp.int32, (2 * FEAT, width), 0) // FEAT
    choice = lax.broadcasted_iota(jnp.int32, (entries, width), 0)

    def some_entries(members):
        sides = []
        starts = []
        for e in members:
            start, order = place[0, e], place[1, e]
            starts.append(start + order * FEAT)
            tile = reply_ref[pl.ds(pl.multiple_of(start, REPLY_ROWS), REPLY_ROWS), :]
            kept = jnp.where(slot == order, tile, 0.0)
            rows = stack_terms(*split3(kept)) + [to_one(choice == e).astype(jnp.bfloat16)]
            sides.append(jnp.concatenate(rows, axis=0))
        gaps = jnp.dot(left_ref[0:first, :], jnp.concatenate(sides, axis=1), preferred_element_type=jnp.float32)
        best_ref[0:first, :] = functools.reduce(
            jnp.minimum, [gaps[:, i * width : (i + 1) * width] for i in range(len(sides))]
        )
        for j in range(first, count, CHUNK):
            here = slice(j - spread_start, j - spread_start + CHUNK)
            x, y, z = [spread_ref[c, here, :] for c in range(3)]
            least = jnp.full((CHUNK, width), penalty, jnp.float32)
            for e, start in zip(members, starts):
                lx, ly, lz, off = [reply_ref[pl.ds(start + c, 1), :] for c in range(FEAT)]
                shade = jnp.broadcast_to(shade_ref[here, e : e + 1], (CHUNK, width))
                least = jnp.minimum(least, ((x * lx + y * ly) + (z * lz + off)) + shade)
            best_ref[j : j + CHUNK, :] = least

    least = 0
    for most in GHOST_LEVELS:
        some = min(most, entries)
        if some > least:
            enough = limit_ref[0] > least if some == entries else (limit_ref[0] > least) & (limit_ref[0] <= some)
            pl.when(enough)(functools.partial(some_entries, range(some)))
        least = some
    px, py, pz = [nodes_ref[c : c + 1, :] for c in range(3)]
    square = px * px + py * py + pz * pz
    own_out_ref[...] = own_ref[...] + square
    for g in range(count // width):
        here = slice(g * width, (g + 1) * width)
        least = jnp.min(best_ref[here, :].T, axis=0, keepdims=True)
        out_ref[:, here] = jnp.minimum(far_gap, least + square[:, here])


def exchange(rows, parts):
    per_part = rows.shape[0] // parts
    shaped = rows.reshape(parts, per_part, 1, rows.shape[1])
    moved = lax.all_to_all(shaped, AXES, split_axis=0, concat_axis=0, tiled=True)
    return moved.reshape(rows.shape)


def local(facets, owner, ghosts, ghost_count, nodes, cand):
    parts = lax.axis_size(AXES)
    blocks, _, width = facets.shape
    count = nodes.shape[1]
    entries = ghosts.shape[1]
    f32 = jnp.float32
    smem = pl.BlockSpec(memory_space=pltpu.SMEM)
    vmem = pl.BlockSpec(memory_space=pltpu.VMEM)
    params = pltpu.CompilerParams(vmem_limit_bytes=16 * 1024 * 1024)
    hbm = pl.BlockSpec(memory_space=pltpu.HBM)
    outgoing, table = pl.pallas_call(
        pack_kernel,
        out_shape=(
            jax.ShapeDtypeStruct((parts * SEND_ROWS, width), f32),
            jax.ShapeDtypeStruct((blocks * FEAT, width), f32),
        ),
        in_specs=[hbm] * 3,
        out_specs=(vmem, vmem),
        scratch_shapes=[
            pltpu.VMEM((12, blocks, width), f32),
            pltpu.VMEM((1, blocks), jnp.int32),
            pltpu.VMEM((1, entries), jnp.int32),
            pltpu.SemaphoreType.DMA((3,)),
        ],
        name="pack",
        compiler_params=params,
    )(*[pltpu.with_memory_space_constraint(v, pltpu.HBM) for v in (jnp.transpose(facets, (1, 0, 2)), owner.T, ghosts)])
    arrived = exchange(outgoing, parts)
    left, spread, shade, place = pl.pallas_call(
        functools.partial(prep_kernel, blocks=blocks),
        out_shape=(
            jax.ShapeDtypeStruct((count, 6 * 2 * FEAT + entries), jnp.bfloat16),
            jax.ShapeDtypeStruct((3, SPREAD, width), f32),
            jax.ShapeDtypeStruct((SPREAD, entries), f32),
            jax.ShapeDtypeStruct((2, entries), jnp.int32),
        ),
        in_specs=[smem, vmem, vmem, vmem],
        out_specs=(vmem, vmem, vmem, vmem),
        name="prep",
        compiler_params=params,
    )(ghost_count, ghosts, nodes, cand)
    answer = pl.pallas_call(
        select_kernel,
        out_shape=jax.ShapeDtypeStruct((parts * REPLY_ROWS, width), f32),
        in_specs=[vmem, vmem],
        out_specs=vmem,
        name="select",
        compiler_params=params,
    )(arrived, table)
    reply = exchange(answer, parts)
    own_least = pl.pallas_call(
        own_kernel,
        out_shape=jax.ShapeDtypeStruct((1, count), f32),
        in_specs=[vmem] * 3,
        out_specs=vmem,
        scratch_shapes=[pltpu.VMEM((count, width), f32)],
        name="own",
        compiler_params=params,
        cost_estimate=pl.CostEstimate(
            flops=7 * parts * CAP * width * count, bytes_accessed=parts * SEND_ROWS * width * 4, transcendentals=0
        ),
    )(arrived, left, spread)
    own_gap, ghost_gap = pl.pallas_call(
        ghost_kernel,
        out_shape=[jax.ShapeDtypeStruct((1, count), f32)] * 2,
        in_specs=[smem] + [vmem] * 7,
        out_specs=[vmem, vmem],
        scratch_shapes=[pltpu.VMEM((count, width), f32)],
        name="ghost",
        compiler_params=params,
    )(ghost_count, place, reply, nodes, left, spread, shade, own_least)
    return own_gap.reshape(count), ghost_gap.reshape(count)


def solution(mesh):
    return jax.shard_map(
        local,
        mesh=mesh,
        in_specs=(
            P(AXES, None, None),
            P(AXES, None),
            P(AXES, None),
            P(AXES),
            P(None, AXES),
            P(None, AXES),
        ),
        out_specs=(P(AXES), P(AXES)),
        check_vma=False,
    )
```

```python
import functools

import jax
import jax.numpy as jnp
from jax import lax
from jax.experimental import pallas as pl
from jax.experimental.pallas import tpu as pltpu
from jax.sharding import PartitionSpec as P

CAP = 4
GC = 2
FEAT = 4
OWN_ROWS = CAP * FEAT
SEND_ROWS = OWN_ROWS + 1
REPLY_ROWS = GC * FEAT
UNROLL = 16
CHUNK = 64
GHOST_CHUNKS = 2
SPREAD = 128
GHOST_LEVELS = (4, 8, 1 << 30)
AXES = ("gx", "gy")

far_gap = 10.0
penalty = 1e30


def split3(value):
    high = value.astype(jnp.bfloat16)
    rest = value - high.astype(jnp.float32)
    middle = rest.astype(jnp.bfloat16)
    low = (rest - middle.astype(jnp.float32)).astype(jnp.bfloat16)
    return high, middle, low


def to_one(flag):
    return jnp.where(flag, 1.0, 0.0)


def pack_kernel(facets_hbm, owner_hbm, ghosts_hbm, out_ref, table_ref, facets_ref, owner_ref, ghosts_ref, sems):
    _, blocks, width = facets_ref.shape
    parts = out_ref.shape[0] // SEND_ROWS
    fetches = [
        pltpu.make_async_copy(source, target, sems.at[i])
        for i, (source, target) in enumerate(
            ((ghosts_hbm, ghosts_ref), (owner_hbm, owner_ref), (facets_hbm, facets_ref))
        )
    ]
    for fetch in fetches:
        fetch.start()
    fetches[0].wait()
    fetches[1].wait()
    owner_row = owner_ref[...]
    row_id = lax.broadcasted_iota(jnp.int32, (blocks, blocks), 0)
    col_id = lax.broadcasted_iota(jnp.int32, (blocks, blocks), 1)
    owner_col = jnp.sum(jnp.where(row_id == col_id, owner_row, 0), axis=1, keepdims=True)
    earlier = (owner_col == owner_row) & (row_id < col_id)
    rank = jnp.sum(jnp.where(earlier, 1, 0), axis=0, keepdims=True)
    places = owner_row * SEND_ROWS + rank * FEAT
    starts = [places[0, b] for b in range(blocks)]
    out_ref[...] = jnp.zeros(out_ref.shape, jnp.float32)
    for slot in range(CAP):
        out_ref[pl.ds(slot * FEAT + FEAT - 1, parts, stride=SEND_ROWS), :] = jnp.full((parts, width), penalty, jnp.float32)

    wanted = ghosts_ref[...]
    entries = wanted.shape[1]
    part_of = lax.broadcasted_iota(jnp.int32, (parts, entries), 0)
    entry = lax.broadcasted_iota(jnp.int32, (parts, entries), 1)
    holder = wanted // blocks
    local_row = wanted - holder * blocks
    held = part_of == holder
    first = jnp.min(jnp.where(held, entry, entries), axis=1, keepdims=True)
    last = jnp.max(jnp.where(held, entry, -1), axis=1, keepdims=True)
    row_first = jnp.sum(jnp.where(held & (entry == first), local_row, 0), axis=1, keepdims=True)
    row_last = jnp.sum(jnp.where(held & (entry == last), local_row, 0), axis=1, keepdims=True)
    lane = lax.broadcasted_iota(jnp.int32, (parts, width), 1)
    request = jnp.where(lane == 0, row_first, jnp.where(lane == 1, row_last, 0))
    out_ref[pl.ds(OWN_ROWS, parts, stride=SEND_ROWS), :] = request.astype(jnp.float32)

    fetches[2].wait()
    ax, ay, az, bx, by, bz, cx, cy, cz, nx, ny, nz = [facets_ref[i] for i in range(12)]
    third = 1.0 / 3.0
    squares = lambda u, v, w: u * u + v * v + w * w
    spread = (squares(ax, bx, cx) + squares(ay, by, cy) + squares(az, bz, cz)) * third
    offset = spread - (nx * ax + ny * ay + nz * az)
    feats = [n - (2.0 * third) * (a + b + c) for n, a, b, c in ((nx, ax, bx, cx), (ny, ay, by, cy), (nz, az, bz, cz))]
    feats.append(offset)
    for c in range(FEAT):
        table_ref[pl.ds(c, blocks, stride=FEAT), :] = feats[c]
    for b in range(blocks):
        out_ref[pl.ds(starts[b], FEAT), :] = table_ref[b * FEAT : (b + 1) * FEAT, :]


def select_kernel(arrived_ref, table_ref, out_ref):
    parts = arrived_ref.shape[0] // SEND_ROWS
    request = arrived_ref[pl.ds(OWN_ROWS, parts, stride=SEND_ROWS), :].astype(jnp.int32) * FEAT
    for d in range(parts):
        for s in range(GC):
            row = d * REPLY_ROWS + s * FEAT
            out_ref[row : row + FEAT, :] = table_ref[pl.ds(pl.multiple_of(request[d, s], FEAT), FEAT), :]


def stack_terms(high, middle, low):
    return [high, high, high, middle, middle, low]


def point_terms(points):
    four = jnp.concatenate([points, jnp.ones_like(points[0:1])], axis=0)
    high, middle, low = [t.astype(jnp.float32) for t in split3(jnp.concatenate([four, four], axis=0))]
    return [high, middle, low, high, middle, high]


def prep_kernel(limit_ref, wanted_ref, nodes_ref, cand_ref, left_ref, spread_ref, shade_ref, place_ref, *, blocks):
    count = nodes_ref.shape[1]
    _, spread_count, width = spread_ref.shape
    start = count - spread_count
    entries = wanted_ref.shape[1]
    holder = wanted_ref[...] // blocks
    row_id = lax.broadcasted_iota(jnp.int32, (entries, entries), 0)
    col_id = lax.broadcasted_iota(jnp.int32, (entries, entries), 1)
    holder_col = jnp.sum(jnp.where(row_id == col_id, holder, 0), axis=1, keepdims=True)
    earlier = (holder_col == holder) & (row_id < col_id)
    order = jnp.sum(jnp.where(earlier, 1, 0), axis=0, keepdims=True)
    place_ref[0:1, :] = holder * REPLY_ROWS
    place_ref[1:2, :] = order
    entry = lax.broadcasted_iota(jnp.int32, (entries, count), 0)
    chosen = entry == cand_ref[0:1, :]
    for k in range(1, cand_ref.shape[0]):
        chosen = chosen | (entry == cand_ref[k : k + 1, :])
    mask = jnp.where(chosen & (entry < limit_ref[0]), 0.0, penalty)
    left_ref[...] = jnp.concatenate(point_terms(nodes_ref[...]) + [mask], axis=0).T.astype(jnp.bfloat16)
    shade_ref[...] = mask[:, start:].T
    for c in range(3):
        for g in range(spread_count // width):
            row = nodes_ref[c : c + 1, start + g * width : start + (g + 1) * width]
            spread_ref[c, g * width : (g + 1) * width, :] = jnp.broadcast_to(row, (width, width)).T


def own_kernel(arrived_ref, left_ref, spread_ref, out_ref, best_ref):
    parts = arrived_ref.shape[0] // SEND_ROWS
    width = arrived_ref.shape[1]
    count = left_ref.shape[0]
    first = count - spread_ref.shape[1]
    entries = left_ref.shape[1] - 6 * 2 * FEAT
    best_ref[...] = jnp.full((count, width), penalty, jnp.float32)
    sublane = lax.broadcasted_iota(jnp.int32, (2 * FEAT, width), 0)
    chunk = CHUNK
    unroll = UNROLL

    def some_sources(i, carry):
        for u in range(unroll):
            base = (i * unroll + u) * SEND_ROWS
            sides = []
            for t in range(CAP // 2):
                tile = arrived_ref[pl.ds(base + t * 2 * FEAT, 2 * FEAT), :]
                for part in range(2):
                    kept = jnp.where((sublane >= FEAT) == (part == 1), tile, 0.0)
                    rows = stack_terms(*split3(kept)) + [jnp.zeros((entries, width), jnp.bfloat16)]
                    sides.append(jnp.concatenate(rows, axis=0))
            gaps = jnp.dot(left_ref[0:first, :], jnp.concatenate(sides, axis=1), preferred_element_type=jnp.float32)
            least = best_ref[0:first, :]
            for s in range(CAP):
                least = jnp.minimum(least, gaps[:, s * width : (s + 1) * width])
            best_ref[0:first, :] = least
            for j in range((count - first) // chunk):
                x, y, z = [spread_ref[c, j * chunk : (j + 1) * chunk, :] for c in range(3)]
                here = slice(first + j * chunk, first + (j + 1) * chunk)
                least = best_ref[here, :]
                for s in range(CAP):
                    lx, ly, lz, off = [arrived_ref[pl.ds(base + s * FEAT + c, 1), :] for c in range(FEAT)]
                    least = jnp.minimum(least, (x * lx + y * ly) + (z * lz + off))
                best_ref[here, :] = least
        return carry

    lax.fori_loop(0, parts // unroll, some_sources, 0)
    for g in range(count // width):
        here = slice(g * width, (g + 1) * width)
        out_ref[:, here] = jnp.min(best_ref[here, :].T, axis=0, keepdims=True)


def ghost_kernel(
    limit_ref, place_ref, reply_ref, nodes_ref, left_ref, spread_ref, shade_ref, own_ref, own_out_ref, out_ref, best_ref
):
    entries = place_ref.shape[1]
    count = nodes_ref.shape[1]
    width = reply_ref.shape[1]
    spread_start = count - spread_ref.shape[1]
    first = count - GHOST_CHUNKS * CHUNK
    place = place_ref[...]
    slot = lax.broadcasted_iota(jnp.int32, (2 * FEAT, width), 0) // FEAT
    choice = lax.broadcasted_iota(jnp.int32, (entries, width), 0)

    def some_entries(members):
        sides = []
        starts = []
        for e in members:
            start, order = place[0, e], place[1, e]
            starts.append(start + order * FEAT)
            tile = reply_ref[pl.ds(pl.multiple_of(start, REPLY_ROWS), REPLY_ROWS), :]
            kept = jnp.where(slot == order, tile, 0.0)
            rows = stack_terms(*split3(kept)) + [to_one(choice == e).astype(jnp.bfloat16)]
            sides.append(jnp.concatenate(rows, axis=0))
        gaps = jnp.dot(left_ref[0:first, :], jnp.concatenate(sides, axis=1), preferred_element_type=jnp.float32)
        best_ref[0:first, :] = functools.reduce(
            jnp.minimum, [gaps[:, i * width : (i + 1) * width] for i in range(len(sides))]
        )
        for j in range(first, count, CHUNK):
            here = slice(j - spread_start, j - spread_start + CHUNK)
            x, y, z = [spread_ref[c, here, :] for c in range(3)]
            least = jnp.full((CHUNK, width), penalty, jnp.float32)
            for e, start in zip(members, starts):
                lx, ly, lz, off = [reply_ref[pl.ds(start + c, 1), :] for c in range(FEAT)]
                shade = jnp.broadcast_to(shade_ref[here, e : e + 1], (CHUNK, width))
                least = jnp.minimum(least, ((x * lx + y * ly) + (z * lz + off)) + shade)
            best_ref[j : j + CHUNK, :] = least

    least = 0
    for most in GHOST_LEVELS:
        some = min(most, entries)
        if some > least:
            fits = limit_ref[0] > least if some == entries else limit_ref[0] <= some
            pl.when(fits if least == 0 else fits & (limit_ref[0] > least))(functools.partial(some_entries, range(some)))
        least = some
    px, py, pz = [nodes_ref[c : c + 1, :] for c in range(3)]
    square = px * px + py * py + pz * pz
    own_out_ref[...] = own_ref[...] + square
    for g in range(count // width):
        here = slice(g * width, (g + 1) * width)
        least = jnp.min(best_ref[here, :].T, axis=0, keepdims=True)
        out_ref[:, here] = jnp.minimum(far_gap, least + square[:, here])


def exchange(rows, parts):
    per_part = rows.shape[0] // parts
    shaped = rows.reshape(parts, per_part, 1, rows.shape[1])
    moved = lax.all_to_all(shaped, AXES, split_axis=0, concat_axis=0, tiled=True)
    return moved.reshape(rows.shape)


def local(facets, owner, ghosts, ghost_count, nodes, cand):
    parts = lax.axis_size(AXES)
    blocks, _, width = facets.shape
    count = nodes.shape[1]
    entries = ghosts.shape[1]
    f32 = jnp.float32
    smem = pl.BlockSpec(memory_space=pltpu.SMEM)
    vmem = pl.BlockSpec(memory_space=pltpu.VMEM)
    params = pltpu.CompilerParams(vmem_limit_bytes=16 * 1024 * 1024)
    hbm = pl.BlockSpec(memory_space=pltpu.HBM)
    outgoing, table = pl.pallas_call(
        pack_kernel,
        out_shape=(
            jax.ShapeDtypeStruct((parts * SEND_ROWS, width), f32),
            jax.ShapeDtypeStruct((blocks * FEAT, width), f32),
        ),
        in_specs=[hbm] * 3,
        out_specs=(vmem, vmem),
        scratch_shapes=[
            pltpu.VMEM((12, blocks, width), f32),
            pltpu.VMEM((1, blocks), jnp.int32),
            pltpu.VMEM((1, entries), jnp.int32),
            pltpu.SemaphoreType.DMA((3,)),
        ],
        name="pack",
        compiler_params=params,
    )(*[pltpu.with_memory_space_constraint(v, pltpu.HBM) for v in (jnp.transpose(facets, (1, 0, 2)), owner.T, ghosts)])
    arrived = exchange(outgoing, parts)
    left, spread, shade, place = pl.pallas_call(
        functools.partial(prep_kernel, blocks=blocks),
        out_shape=(
            jax.ShapeDtypeStruct((count, 6 * 2 * FEAT + entries), jnp.bfloat16),
            jax.ShapeDtypeStruct((3, SPREAD, width), f32),
            jax.ShapeDtypeStruct((SPREAD, entries), f32),
            jax.ShapeDtypeStruct((2, entries), jnp.int32),
        ),
        in_specs=[smem, vmem, vmem, vmem],
        out_specs=(vmem, vmem, vmem, vmem),
        name="prep",
        compiler_params=params,
    )(ghost_count, ghosts, nodes, cand)
    answer = pl.pallas_call(
        select_kernel,
        out_shape=jax.ShapeDtypeStruct((parts * REPLY_ROWS, width), f32),
        in_specs=[vmem, vmem],
        out_specs=vmem,
        name="select",
        compiler_params=params,
    )(arrived, table)
    reply = exchange(answer, parts)
    own_least = pl.pallas_call(
        own_kernel,
        out_shape=jax.ShapeDtypeStruct((1, count), f32),
        in_specs=[vmem] * 3,
        out_specs=vmem,
        scratch_shapes=[pltpu.VMEM((count, width), f32)],
        name="own",
        compiler_params=params,
        cost_estimate=pl.CostEstimate(
            flops=7 * parts * CAP * width * count, bytes_accessed=parts * SEND_ROWS * width * 4, transcendentals=0
        ),
    )(arrived, left, spread)
    own_gap, ghost_gap = pl.pallas_call(
        ghost_kernel,
        out_shape=[jax.ShapeDtypeStruct((1, count), f32)] * 2,
        in_specs=[smem] + [vmem] * 7,
        out_specs=[vmem, vmem],
        scratch_shapes=[pltpu.VMEM((count, width), f32)],
        name="ghost",
        compiler_params=params,
    )(ghost_count, place, reply, nodes, left, spread, shade, own_least)
    return own_gap.reshape(count), ghost_gap.reshape(count)


def solution(mesh):
    return jax.shard_map(
        local,
        mesh=mesh,
        in_specs=(
            P(AXES, None, None),
            P(AXES, None),
            P(AXES, None),
            P(AXES),
            P(None, AXES),
            P(None, AXES),
        ),
        out_specs=(P(AXES), P(AXES)),
        check_vma=False,
    )
```

```python
import functools

import jax
import jax.numpy as jnp
from jax import lax
from jax.experimental import pallas as pl
from jax.experimental.pallas import tpu as pltpu
from jax.sharding import PartitionSpec as P

CAP = 4
GC = 2
FEAT = 4
OWN_ROWS = CAP * FEAT
SEND_ROWS = OWN_ROWS + 1
REPLY_ROWS = GC * FEAT
UNROLL = 16
CHUNK = 64
SPREAD = 128
GHOST_LEVELS = (2, 4, 8, 12, 1 << 30)
AXES = ("gx", "gy")

far_gap = 10.0
penalty = 1e30


def split3(value):
    high = value.astype(jnp.bfloat16)
    rest = value - high.astype(jnp.float32)
    middle = rest.astype(jnp.bfloat16)
    low = (rest - middle.astype(jnp.float32)).astype(jnp.bfloat16)
    return high, middle, low


def to_one(flag):
    return jnp.where(flag, 1.0, 0.0)


def pack_kernel(facets_hbm, owner_hbm, ghosts_hbm, out_ref, table_ref, facets_ref, owner_ref, ghosts_ref, sems):
    _, blocks, width = facets_ref.shape
    parts = out_ref.shape[0] // SEND_ROWS
    fetches = [
        pltpu.make_async_copy(source, target, sems.at[i])
        for i, (source, target) in enumerate(
            ((ghosts_hbm, ghosts_ref), (owner_hbm, owner_ref), (facets_hbm, facets_ref))
        )
    ]
    for fetch in fetches:
        fetch.start()
    fetches[0].wait()
    fetches[1].wait()
    owner_row = owner_ref[...]
    row_id = lax.broadcasted_iota(jnp.int32, (blocks, blocks), 0)
    col_id = lax.broadcasted_iota(jnp.int32, (blocks, blocks), 1)
    owner_col = jnp.sum(jnp.where(row_id == col_id, owner_row, 0), axis=1, keepdims=True)
    earlier = (owner_col == owner_row) & (row_id < col_id)
    rank = jnp.sum(jnp.where(earlier, 1, 0), axis=0, keepdims=True)
    places = owner_row * SEND_ROWS + rank * FEAT
    starts = [places[0, b] for b in range(blocks)]
    out_ref[...] = jnp.zeros(out_ref.shape, jnp.float32)
    for slot in range(CAP):
        out_ref[pl.ds(slot * FEAT + FEAT - 1, parts, stride=SEND_ROWS), :] = jnp.full((parts, width), penalty, jnp.float32)

    wanted = ghosts_ref[...]
    entries = wanted.shape[1]
    part_of = lax.broadcasted_iota(jnp.int32, (parts, entries), 0)
    entry = lax.broadcasted_iota(jnp.int32, (parts, entries), 1)
    holder = wanted // blocks
    local_row = wanted - holder * blocks
    held = part_of == holder
    first = jnp.min(jnp.where(held, entry, entries), axis=1, keepdims=True)
    last = jnp.max(jnp.where(held, entry, -1), axis=1, keepdims=True)
    row_first = jnp.sum(jnp.where(held & (entry == first), local_row, 0), axis=1, keepdims=True)
    row_last = jnp.sum(jnp.where(held & (entry == last), local_row, 0), axis=1, keepdims=True)
    lane = lax.broadcasted_iota(jnp.int32, (parts, width), 1)
    request = jnp.where(lane == 0, row_first, jnp.where(lane == 1, row_last, 0))
    out_ref[pl.ds(OWN_ROWS, parts, stride=SEND_ROWS), :] = request.astype(jnp.float32)

    fetches[2].wait()
    ax, ay, az, bx, by, bz, cx, cy, cz, nx, ny, nz = [facets_ref[i] for i in range(12)]
    third = 1.0 / 3.0
    squares = lambda u, v, w: u * u + v * v + w * w
    spread = (squares(ax, bx, cx) + squares(ay, by, cy) + squares(az, bz, cz)) * third
    offset = spread - (nx * ax + ny * ay + nz * az)
    feats = [n - (2.0 * third) * (a + b + c) for n, a, b, c in ((nx, ax, bx, cx), (ny, ay, by, cy), (nz, az, bz, cz))]
    feats.append(offset)
    for c in range(FEAT):
        table_ref[pl.ds(c, blocks, stride=FEAT), :] = feats[c]
    for b in range(blocks):
        out_ref[pl.ds(starts[b], FEAT), :] = table_ref[b * FEAT : (b + 1) * FEAT, :]


def select_kernel(arrived_ref, table_ref, out_ref):
    parts = arrived_ref.shape[0] // SEND_ROWS
    request = arrived_ref[pl.ds(OWN_ROWS, parts, stride=SEND_ROWS), :].astype(jnp.int32) * FEAT
    for d in range(parts):
        for s in range(GC):
            row = d * REPLY_ROWS + s * FEAT
            out_ref[row : row + FEAT, :] = table_ref[pl.ds(pl.multiple_of(request[d, s], FEAT), FEAT), :]


def stack_terms(high, middle, low):
    return [high, high, high, middle, middle, low]


def point_terms(points):
    four = jnp.concatenate([points, jnp.ones_like(points[0:1])], axis=0)
    high, middle, low = [t.astype(jnp.float32) for t in split3(jnp.concatenate([four, four], axis=0))]
    return [high, middle, low, high, middle, high]


def prep_kernel(limit_ref, wanted_ref, nodes_ref, cand_ref, left_ref, right_ref, spread_ref, place_ref, *, blocks):
    count = nodes_ref.shape[1]
    _, spread_count, width = spread_ref.shape
    start = count - spread_count
    entries = wanted_ref.shape[1]
    holder = wanted_ref[...] // blocks
    row_id = lax.broadcasted_iota(jnp.int32, (entries, entries), 0)
    col_id = lax.broadcasted_iota(jnp.int32, (entries, entries), 1)
    holder_col = jnp.sum(jnp.where(row_id == col_id, holder, 0), axis=1, keepdims=True)
    earlier = (holder_col == holder) & (row_id < col_id)
    order = jnp.sum(jnp.where(earlier, 1, 0), axis=0, keepdims=True)
    place_ref[0:1, :] = holder * REPLY_ROWS
    place_ref[1:2, :] = order
    entry = lax.broadcasted_iota(jnp.int32, (entries, count), 0)
    chosen = entry == cand_ref[0:1, :]
    for k in range(1, cand_ref.shape[0]):
        chosen = chosen | (entry == cand_ref[k : k + 1, :])
    mask = jnp.where(chosen & (entry < limit_ref[0]), 0.0, penalty)
    right = jnp.concatenate(point_terms(nodes_ref[...]) + [mask], axis=0)
    right_ref[...] = right.astype(jnp.bfloat16)
    left_ref[...] = right.T.astype(jnp.bfloat16)
    for c in range(3):
        for g in range(spread_count // width):
            row = nodes_ref[c : c + 1, start + g * width : start + (g + 1) * width]
            spread_ref[c, g * width : (g + 1) * width, :] = jnp.broadcast_to(row, (width, width)).T


def own_kernel(arrived_ref, left_ref, spread_ref, out_ref, best_ref):
    parts = arrived_ref.shape[0] // SEND_ROWS
    width = arrived_ref.shape[1]
    count = left_ref.shape[0]
    first = count - spread_ref.shape[1]
    entries = left_ref.shape[1] - 6 * 2 * FEAT
    best_ref[...] = jnp.full((count, width), penalty, jnp.float32)
    sublane = lax.broadcasted_iota(jnp.int32, (2 * FEAT, width), 0)
    chunk = CHUNK
    unroll = UNROLL

    def some_sources(i, carry):
        for u in range(unroll):
            base = (i * unroll + u) * SEND_ROWS
            sides = []
            for t in range(CAP // 2):
                tile = arrived_ref[pl.ds(base + t * 2 * FEAT, 2 * FEAT), :]
                for part in range(2):
                    kept = jnp.where((sublane >= FEAT) == (part == 1), tile, 0.0)
                    rows = stack_terms(*split3(kept)) + [jnp.zeros((entries, width), jnp.bfloat16)]
                    sides.append(jnp.concatenate(rows, axis=0))
            gaps = jnp.dot(left_ref[0:first, :], jnp.concatenate(sides, axis=1), preferred_element_type=jnp.float32)
            least = best_ref[0:first, :]
            for s in range(CAP):
                least = jnp.minimum(least, gaps[:, s * width : (s + 1) * width])
            best_ref[0:first, :] = least
            for j in range((count - first) // chunk):
                x, y, z = [spread_ref[c, j * chunk : (j + 1) * chunk, :] for c in range(3)]
                here = slice(first + j * chunk, first + (j + 1) * chunk)
                least = best_ref[here, :]
                for s in range(CAP):
                    lx, ly, lz, off = [arrived_ref[pl.ds(base + s * FEAT + c, 1), :] for c in range(FEAT)]
                    least = jnp.minimum(least, (x * lx + y * ly) + (z * lz + off))
                best_ref[here, :] = least
        return carry

    lax.fori_loop(0, parts // unroll, some_sources, 0)
    for g in range(count // width):
        here = slice(g * width, (g + 1) * width)
        out_ref[:, here] = jnp.min(best_ref[here, :].T, axis=0, keepdims=True)


def ghost_kernel(limit_ref, place_ref, reply_ref, nodes_ref, right_ref, own_ref, own_out_ref, out_ref, best_ref):
    entries = place_ref.shape[1]
    count = nodes_ref.shape[1]
    width = reply_ref.shape[1]
    place = place_ref[...]
    slot = lax.broadcasted_iota(jnp.int32, (2 * FEAT, width), 0) // FEAT
    choice = lax.broadcasted_iota(jnp.int32, (entries, width), 0)

    def some_entries(members):
        best = None
        for e in members:
            start, order = place[0, e], place[1, e]
            tile = reply_ref[pl.ds(pl.multiple_of(start, REPLY_ROWS), REPLY_ROWS), :]
            kept = jnp.where(slot == order, tile, 0.0)
            rows = jnp.concatenate(stack_terms(*split3(kept)) + [to_one(choice == e).astype(jnp.bfloat16)], axis=0)
            gaps = jnp.dot(rows.T, right_ref[...], preferred_element_type=jnp.float32)
            least = jnp.min(gaps.reshape(width // 8, 8, count), axis=0)
            best = least if best is None else jnp.minimum(best, least)
        best_ref[...] = best

    least = 0
    for most in GHOST_LEVELS:
        some = min(most, entries)
        if some > least:
            fits = limit_ref[0] > least if some == entries else limit_ref[0] <= some
            pl.when(fits if least == 0 else fits & (limit_ref[0] > least))(functools.partial(some_entries, range(some)))
        least = some
    px, py, pz = [nodes_ref[c : c + 1, :] for c in range(3)]
    square = px * px + py * py + pz * pz
    own_out_ref[...] = own_ref[...] + square
    out_ref[...] = jnp.minimum(far_gap, jnp.min(best_ref[...], axis=0, keepdims=True) + square)


def exchange(rows, parts):
    per_part = rows.shape[0] // parts
    shaped = rows.reshape(parts, per_part, 1, rows.shape[1])
    moved = lax.all_to_all(shaped, AXES, split_axis=0, concat_axis=0, tiled=True)
    return moved.reshape(rows.shape)


def local(facets, owner, ghosts, ghost_count, nodes, cand):
    parts = lax.axis_size(AXES)
    blocks, _, width = facets.shape
    count = nodes.shape[1]
    entries = ghosts.shape[1]
    f32 = jnp.float32
    smem = pl.BlockSpec(memory_space=pltpu.SMEM)
    vmem = pl.BlockSpec(memory_space=pltpu.VMEM)
    params = pltpu.CompilerParams(vmem_limit_bytes=16 * 1024 * 1024)
    hbm = pl.BlockSpec(memory_space=pltpu.HBM)
    outgoing, table = pl.pallas_call(
        pack_kernel,
        out_shape=(
            jax.ShapeDtypeStruct((parts * SEND_ROWS, width), f32),
            jax.ShapeDtypeStruct((blocks * FEAT, width), f32),
        ),
        in_specs=[hbm] * 3,
        out_specs=(vmem, vmem),
        scratch_shapes=[
            pltpu.VMEM((12, blocks, width), f32),
            pltpu.VMEM((1, blocks), jnp.int32),
            pltpu.VMEM((1, entries), jnp.int32),
            pltpu.SemaphoreType.DMA((3,)),
        ],
        name="pack",
        compiler_params=params,
    )(*[pltpu.with_memory_space_constraint(v, pltpu.HBM) for v in (jnp.transpose(facets, (1, 0, 2)), owner.T, ghosts)])
    arrived = exchange(outgoing, parts)
    left, right, spread, place = pl.pallas_call(
        functools.partial(prep_kernel, blocks=blocks),
        out_shape=(
            jax.ShapeDtypeStruct((count, 6 * 2 * FEAT + entries), jnp.bfloat16),
            jax.ShapeDtypeStruct((6 * 2 * FEAT + entries, count), jnp.bfloat16),
            jax.ShapeDtypeStruct((3, SPREAD, width), f32),
            jax.ShapeDtypeStruct((2, entries), jnp.int32),
        ),
        in_specs=[smem, vmem, vmem, vmem],
        out_specs=(vmem, vmem, vmem, vmem),
        name="prep",
        compiler_params=params,
    )(ghost_count, ghosts, nodes, cand)
    answer = pl.pallas_call(
        select_kernel,
        out_shape=jax.ShapeDtypeStruct((parts * REPLY_ROWS, width), f32),
        in_specs=[vmem, vmem],
        out_specs=vmem,
        name="select",
        compiler_params=params,
    )(arrived, table)
    reply = exchange(answer, parts)
    own_least = pl.pallas_call(
        own_kernel,
        out_shape=jax.ShapeDtypeStruct((1, count), f32),
        in_specs=[vmem] * 3,
        out_specs=vmem,
        scratch_shapes=[pltpu.VMEM((count, width), f32)],
        name="own",
        compiler_params=params,
        cost_estimate=pl.CostEstimate(
            flops=7 * parts * CAP * width * count, bytes_accessed=parts * SEND_ROWS * width * 4, transcendentals=0
        ),
    )(arrived, left, spread)
    own_gap, ghost_gap = pl.pallas_call(
        ghost_kernel,
        out_shape=[jax.ShapeDtypeStruct((1, count), f32)] * 2,
        in_specs=[smem] + [vmem] * 5,
        out_specs=[vmem, vmem],
        scratch_shapes=[pltpu.VMEM((8, count), f32)],
        name="ghost",
        compiler_params=params,
    )(ghost_count, place, reply, nodes, right, own_least)
    return own_gap.reshape(count), ghost_gap.reshape(count)


def solution(mesh):
    return jax.shard_map(
        local,
        mesh=mesh,
        in_specs=(
            P(AXES, None, None),
            P(AXES, None),
            P(AXES, None),
            P(AXES),
            P(None, AXES),
            P(None, AXES),
        ),
        out_specs=(P(AXES), P(AXES)),
        check_vma=False,
    )
```

```python
import functools

import jax
import jax.numpy as jnp
from jax import lax
from jax.experimental import pallas as pl
from jax.experimental.pallas import tpu as pltpu
from jax.sharding import PartitionSpec as P

CAP = 4
GC = 2
FEAT = 4
OWN_ROWS = CAP * FEAT
SEND_ROWS = OWN_ROWS + 1
REPLY_ROWS = GC * FEAT
UNROLL = 16
CHUNK = 64
GHOST_CHUNKS = 2
SPREAD = 128
GHOST_LEVELS = (2, 4, 8, 12, 1 << 30)
FEW = 8
AXES = ("gx", "gy")

far_gap = 10.0
penalty = 1e30


def split3(value):
    high = value.astype(jnp.bfloat16)
    rest = value - high.astype(jnp.float32)
    middle = rest.astype(jnp.bfloat16)
    low = (rest - middle.astype(jnp.float32)).astype(jnp.bfloat16)
    return high, middle, low


def to_one(flag):
    return jnp.where(flag, 1.0, 0.0)


def pack_kernel(facets_hbm, owner_hbm, ghosts_hbm, out_ref, table_ref, facets_ref, owner_ref, ghosts_ref, sems):
    _, blocks, width = facets_ref.shape
    parts = out_ref.shape[0] // SEND_ROWS
    fetches = [
        pltpu.make_async_copy(source, target, sems.at[i])
        for i, (source, target) in enumerate(
            ((ghosts_hbm, ghosts_ref), (owner_hbm, owner_ref), (facets_hbm, facets_ref))
        )
    ]
    for fetch in fetches:
        fetch.start()
    fetches[0].wait()
    fetches[1].wait()
    owner_row = owner_ref[...]
    row_id = lax.broadcasted_iota(jnp.int32, (blocks, blocks), 0)
    col_id = lax.broadcasted_iota(jnp.int32, (blocks, blocks), 1)
    owner_col = jnp.sum(jnp.where(row_id == col_id, owner_row, 0), axis=1, keepdims=True)
    earlier = (owner_col == owner_row) & (row_id < col_id)
    rank = jnp.sum(jnp.where(earlier, 1, 0), axis=0, keepdims=True)
    places = owner_row * SEND_ROWS + rank * FEAT
    starts = [places[0, b] for b in range(blocks)]
    out_ref[...] = jnp.zeros(out_ref.shape, jnp.float32)
    for slot in range(CAP):
        out_ref[pl.ds(slot * FEAT + FEAT - 1, parts, stride=SEND_ROWS), :] = jnp.full((parts, width), penalty, jnp.float32)

    wanted = ghosts_ref[...]
    entries = wanted.shape[1]
    part_of = lax.broadcasted_iota(jnp.int32, (parts, entries), 0)
    entry = lax.broadcasted_iota(jnp.int32, (parts, entries), 1)
    holder = wanted // blocks
    local_row = wanted - holder * blocks
    held = part_of == holder
    first = jnp.min(jnp.where(held, entry, entries), axis=1, keepdims=True)
    last = jnp.max(jnp.where(held, entry, -1), axis=1, keepdims=True)
    row_first = jnp.sum(jnp.where(held & (entry == first), local_row, 0), axis=1, keepdims=True)
    row_last = jnp.sum(jnp.where(held & (entry == last), local_row, 0), axis=1, keepdims=True)
    lane = lax.broadcasted_iota(jnp.int32, (parts, width), 1)
    request = jnp.where(lane == 0, row_first, jnp.where(lane == 1, row_last, 0))
    out_ref[pl.ds(OWN_ROWS, parts, stride=SEND_ROWS), :] = request.astype(jnp.float32)

    fetches[2].wait()
    ax, ay, az, bx, by, bz, cx, cy, cz, nx, ny, nz = [facets_ref[i] for i in range(12)]
    third = 1.0 / 3.0
    squares = lambda u, v, w: u * u + v * v + w * w
    spread = (squares(ax, bx, cx) + squares(ay, by, cy) + squares(az, bz, cz)) * third
    offset = spread - (nx * ax + ny * ay + nz * az)
    feats = [n - (2.0 * third) * (a + b + c) for n, a, b, c in ((nx, ax, bx, cx), (ny, ay, by, cy), (nz, az, bz, cz))]
    feats.append(offset)
    for c in range(FEAT):
        table_ref[pl.ds(c, blocks, stride=FEAT), :] = feats[c]
    for b in range(blocks):
        out_ref[pl.ds(starts[b], FEAT), :] = table_ref[b * FEAT : (b + 1) * FEAT, :]


def select_kernel(arrived_ref, table_ref, out_ref):
    parts = arrived_ref.shape[0] // SEND_ROWS
    request = arrived_ref[pl.ds(OWN_ROWS, parts, stride=SEND_ROWS), :].astype(jnp.int32) * FEAT
    for d in range(parts):
        for s in range(GC):
            row = d * REPLY_ROWS + s * FEAT
            out_ref[row : row + FEAT, :] = table_ref[pl.ds(pl.multiple_of(request[d, s], FEAT), FEAT), :]


def stack_terms(high, middle, low):
    return [high, high, high, middle, middle, low]


def point_terms(points):
    four = jnp.concatenate([points, jnp.ones_like(points[0:1])], axis=0)
    high, middle, low = [t.astype(jnp.float32) for t in split3(jnp.concatenate([four, four], axis=0))]
    return [high, middle, low, high, middle, high]


def prep_kernel(limit_ref, wanted_ref, nodes_ref, cand_ref, left_ref, right_ref, spread_ref, shade_ref, place_ref, *, blocks):
    count = nodes_ref.shape[1]
    _, spread_count, width = spread_ref.shape
    start = count - spread_count
    entries = wanted_ref.shape[1]
    holder = wanted_ref[...] // blocks
    row_id = lax.broadcasted_iota(jnp.int32, (entries, entries), 0)
    col_id = lax.broadcasted_iota(jnp.int32, (entries, entries), 1)
    holder_col = jnp.sum(jnp.where(row_id == col_id, holder, 0), axis=1, keepdims=True)
    earlier = (holder_col == holder) & (row_id < col_id)
    order = jnp.sum(jnp.where(earlier, 1, 0), axis=0, keepdims=True)
    place_ref[0:1, :] = holder * REPLY_ROWS
    place_ref[1:2, :] = order
    entry = lax.broadcasted_iota(jnp.int32, (entries, count), 0)
    chosen = entry == cand_ref[0:1, :]
    for k in range(1, cand_ref.shape[0]):
        chosen = chosen | (entry == cand_ref[k : k + 1, :])
    mask = jnp.where(chosen & (entry < limit_ref[0]), 0.0, penalty)
    right = jnp.concatenate(point_terms(nodes_ref[...]) + [mask], axis=0)
    right_ref[...] = right.astype(jnp.bfloat16)
    left_ref[...] = right.T.astype(jnp.bfloat16)
    shade_ref[...] = mask[:, start:].T
    for c in range(3):
        for g in range(spread_count // width):
            row = nodes_ref[c : c + 1, start + g * width : start + (g + 1) * width]
            spread_ref[c, g * width : (g + 1) * width, :] = jnp.broadcast_to(row, (width, width)).T


def own_kernel(arrived_ref, left_ref, spread_ref, out_ref, best_ref):
    parts = arrived_ref.shape[0] // SEND_ROWS
    width = arrived_ref.shape[1]
    count = left_ref.shape[0]
    first = count - spread_ref.shape[1]
    entries = left_ref.shape[1] - 6 * 2 * FEAT
    best_ref[...] = jnp.full((count, width), penalty, jnp.float32)
    sublane = lax.broadcasted_iota(jnp.int32, (2 * FEAT, width), 0)
    chunk = CHUNK
    unroll = UNROLL

    def some_sources(i, carry):
        for u in range(unroll):
            base = (i * unroll + u) * SEND_ROWS
            sides = []
            for t in range(CAP // 2):
                tile = arrived_ref[pl.ds(base + t * 2 * FEAT, 2 * FEAT), :]
                for part in range(2):
                    kept = jnp.where((sublane >= FEAT) == (part == 1), tile, 0.0)
                    rows = stack_terms(*split3(kept)) + [jnp.zeros((entries, width), jnp.bfloat16)]
                    sides.append(jnp.concatenate(rows, axis=0))
            gaps = jnp.dot(left_ref[0:first, :], jnp.concatenate(sides, axis=1), preferred_element_type=jnp.float32)
            least = best_ref[0:first, :]
            for s in range(CAP):
                least = jnp.minimum(least, gaps[:, s * width : (s + 1) * width])
            best_ref[0:first, :] = least
            for j in range((count - first) // chunk):
                x, y, z = [spread_ref[c, j * chunk : (j + 1) * chunk, :] for c in range(3)]
                here = slice(first + j * chunk, first + (j + 1) * chunk)
                least = best_ref[here, :]
                for s in range(CAP):
                    lx, ly, lz, off = [arrived_ref[pl.ds(base + s * FEAT + c, 1), :] for c in range(FEAT)]
                    least = jnp.minimum(least, (x * lx + y * ly) + (z * lz + off))
                best_ref[here, :] = least
        return carry

    lax.fori_loop(0, parts // unroll, some_sources, 0)
    for g in range(count // width):
        here = slice(g * width, (g + 1) * width)
        out_ref[:, here] = jnp.min(best_ref[here, :].T, axis=0, keepdims=True)


def ghost_kernel(
    limit_ref, place_ref, reply_ref, nodes_ref, left_ref, right_ref, spread_ref, shade_ref, own_ref, own_out_ref, out_ref, best_ref
):
    entries = place_ref.shape[1]
    count = nodes_ref.shape[1]
    width = reply_ref.shape[1]
    spread_start = count - spread_ref.shape[1]
    first = count - GHOST_CHUNKS * CHUNK
    place = place_ref[...]
    slot = lax.broadcasted_iota(jnp.int32, (2 * FEAT, width), 0) // FEAT
    choice = lax.broadcasted_iota(jnp.int32, (entries, width), 0)

    px, py, pz = [nodes_ref[c : c + 1, :] for c in range(3)]
    square = px * px + py * py + pz * pz
    own_out_ref[...] = own_ref[...] + square

    def few_entries(members):
        best = []
        for e in members:
            tile = reply_ref[pl.ds(pl.multiple_of(place[0, e], REPLY_ROWS), REPLY_ROWS), :]
            kept = jnp.where(slot == place[1, e], tile, 0.0)
            rows = jnp.concatenate(stack_terms(*split3(kept)) + [to_one(choice == e).astype(jnp.bfloat16)], axis=0)
            gaps = jnp.dot(rows.T, right_ref[...], preferred_element_type=jnp.float32)
            best.append(jnp.min(gaps.reshape(width // 8, 8, count), axis=0))
        least = jnp.min(functools.reduce(jnp.minimum, best), axis=0, keepdims=True)
        out_ref[...] = jnp.minimum(far_gap, least + square)

    def some_entries(members):
        sides = []
        starts = []
        for e in members:
            start, order = place[0, e], place[1, e]
            starts.append(start + order * FEAT)
            tile = reply_ref[pl.ds(pl.multiple_of(start, REPLY_ROWS), REPLY_ROWS), :]
            kept = jnp.where(slot == order, tile, 0.0)
            rows = stack_terms(*split3(kept)) + [to_one(choice == e).astype(jnp.bfloat16)]
            sides.append(jnp.concatenate(rows, axis=0))
        gaps = jnp.dot(left_ref[0:first, :], jnp.concatenate(sides, axis=1), preferred_element_type=jnp.float32)
        best_ref[0:first, :] = functools.reduce(
            jnp.minimum, [gaps[:, i * width : (i + 1) * width] for i in range(len(sides))]
        )
        for j in range(first, count, CHUNK):
            here = slice(j - spread_start, j - spread_start + CHUNK)
            x, y, z = [spread_ref[c, here, :] for c in range(3)]
            least = jnp.full((CHUNK, width), penalty, jnp.float32)
            for e, start in zip(members, starts):
                lx, ly, lz, off = [reply_ref[pl.ds(start + c, 1), :] for c in range(FEAT)]
                shade = jnp.broadcast_to(shade_ref[here, e : e + 1], (CHUNK, width))
                least = jnp.minimum(least, ((x * lx + y * ly) + (z * lz + off)) + shade)
            best_ref[j : j + CHUNK, :] = least
        for g in range(count // width):
            here = slice(g * width, (g + 1) * width)
            least = jnp.min(best_ref[here, :].T, axis=0, keepdims=True)
            out_ref[:, here] = jnp.minimum(far_gap, least + square[:, here])

    least = 0
    for most in GHOST_LEVELS:
        some = min(most, entries)
        if some > least:
            fits = limit_ref[0] > least if some == entries else limit_ref[0] <= some
            pl.when(fits if least == 0 else fits & (limit_ref[0] > least))(
                functools.partial(few_entries if some <= FEW else some_entries, range(some))
            )
        least = some


def exchange(rows, parts):
    per_part = rows.shape[0] // parts
    shaped = rows.reshape(parts, per_part, 1, rows.shape[1])
    moved = lax.all_to_all(shaped, AXES, split_axis=0, concat_axis=0, tiled=True)
    return moved.reshape(rows.shape)


def local(facets, owner, ghosts, ghost_count, nodes, cand):
    parts = lax.axis_size(AXES)
    blocks, _, width = facets.shape
    count = nodes.shape[1]
    entries = ghosts.shape[1]
    f32 = jnp.float32
    smem = pl.BlockSpec(memory_space=pltpu.SMEM)
    vmem = pl.BlockSpec(memory_space=pltpu.VMEM)
    params = pltpu.CompilerParams(vmem_limit_bytes=16 * 1024 * 1024)
    hbm = pl.BlockSpec(memory_space=pltpu.HBM)
    outgoing, table = pl.pallas_call(
        pack_kernel,
        out_shape=(
            jax.ShapeDtypeStruct((parts * SEND_ROWS, width), f32),
            jax.ShapeDtypeStruct((blocks * FEAT, width), f32),
        ),
        in_specs=[hbm] * 3,
        out_specs=(vmem, vmem),
        scratch_shapes=[
            pltpu.VMEM((12, blocks, width), f32),
            pltpu.VMEM((1, blocks), jnp.int32),
            pltpu.VMEM((1, entries), jnp.int32),
            pltpu.SemaphoreType.DMA((3,)),
        ],
        name="pack",
        compiler_params=params,
    )(*[pltpu.with_memory_space_constraint(v, pltpu.HBM) for v in (jnp.transpose(facets, (1, 0, 2)), owner.T, ghosts)])
    arrived = exchange(outgoing, parts)
    left, right, spread, shade, place = pl.pallas_call(
        functools.partial(prep_kernel, blocks=blocks),
        out_shape=(
            jax.ShapeDtypeStruct((count, 6 * 2 * FEAT + entries), jnp.bfloat16),
            jax.ShapeDtypeStruct((6 * 2 * FEAT + entries, count), jnp.bfloat16),
            jax.ShapeDtypeStruct((3, SPREAD, width), f32),
            jax.ShapeDtypeStruct((SPREAD, entries), f32),
            jax.ShapeDtypeStruct((2, entries), jnp.int32),
        ),
        in_specs=[smem, vmem, vmem, vmem],
        out_specs=(vmem,) * 5,
        name="prep",
        compiler_params=params,
    )(ghost_count, ghosts, nodes, cand)
    answer = pl.pallas_call(
        select_kernel,
        out_shape=jax.ShapeDtypeStruct((parts * REPLY_ROWS, width), f32),
        in_specs=[vmem, vmem],
        out_specs=vmem,
        name="select",
        compiler_params=params,
    )(arrived, table)
    reply = exchange(answer, parts)
    own_least = pl.pallas_call(
        own_kernel,
        out_shape=jax.ShapeDtypeStruct((1, count), f32),
        in_specs=[vmem] * 3,
        out_specs=vmem,
        scratch_shapes=[pltpu.VMEM((count, width), f32)],
        name="own",
        compiler_params=params,
        cost_estimate=pl.CostEstimate(
            flops=7 * parts * CAP * width * count, bytes_accessed=parts * SEND_ROWS * width * 4, transcendentals=0
        ),
    )(arrived, left, spread)
    own_gap, ghost_gap = pl.pallas_call(
        ghost_kernel,
        out_shape=[jax.ShapeDtypeStruct((1, count), f32)] * 2,
        in_specs=[smem] + [vmem] * 8,
        out_specs=[vmem, vmem],
        scratch_shapes=[pltpu.VMEM((count, width), f32)],
        name="ghost",
        compiler_params=params,
    )(ghost_count, place, reply, nodes, left, right, spread, shade, own_least)
    return own_gap.reshape(count), ghost_gap.reshape(count)


def solution(mesh):
    return jax.shard_map(
        local,
        mesh=mesh,
        in_specs=(
            P(AXES, None, None),
            P(AXES, None),
            P(AXES, None),
            P(AXES),
            P(None, AXES),
            P(None, AXES),
        ),
        out_specs=(P(AXES), P(AXES)),
        check_vma=False,
    )
```

```python
import functools

import jax
import jax.numpy as jnp
from jax import lax
from jax.experimental import pallas as pl
from jax.experimental.pallas import tpu as pltpu
from jax.sharding import PartitionSpec as P

CAP = 4
GC = 2
FEAT = 4
OWN_ROWS = CAP * FEAT
SEND_ROWS = OWN_ROWS + 1
REPLY_ROWS = GC * FEAT
UNROLL = 16
PIECES = 2
CHUNK = 64
GHOST_CHUNKS = 2
SPREAD = 128
GHOST_LEVELS = (2, 4, 8, 12, 1 << 30)
FEW = 8
AXES = ("gx", "gy")

far_gap = 10.0
penalty = 1e30


def split3(value):
    high = value.astype(jnp.bfloat16)
    rest = value - high.astype(jnp.float32)
    middle = rest.astype(jnp.bfloat16)
    low = (rest - middle.astype(jnp.float32)).astype(jnp.bfloat16)
    return high, middle, low


def to_one(flag):
    return jnp.where(flag, 1.0, 0.0)


def pack_kernel(facets_hbm, owner_hbm, ghosts_hbm, out_ref, table_ref, facets_ref, owner_ref, ghosts_ref, sems):
    _, blocks, width = facets_ref.shape
    parts = out_ref.shape[0] // SEND_ROWS
    fetches = [
        pltpu.make_async_copy(source, target, sems.at[i])
        for i, (source, target) in enumerate(
            ((ghosts_hbm, ghosts_ref), (owner_hbm, owner_ref), (facets_hbm, facets_ref))
        )
    ]
    for fetch in fetches:
        fetch.start()
    fetches[0].wait()
    fetches[1].wait()
    owner_row = owner_ref[...]
    row_id = lax.broadcasted_iota(jnp.int32, (blocks, blocks), 0)
    col_id = lax.broadcasted_iota(jnp.int32, (blocks, blocks), 1)
    owner_col = jnp.sum(jnp.where(row_id == col_id, owner_row, 0), axis=1, keepdims=True)
    earlier = (owner_col == owner_row) & (row_id < col_id)
    rank = jnp.sum(jnp.where(earlier, 1, 0), axis=0, keepdims=True)
    places = owner_row * SEND_ROWS + rank * FEAT
    starts = [places[0, b] for b in range(blocks)]
    out_ref[...] = jnp.zeros(out_ref.shape, jnp.float32)
    for slot in range(CAP):
        out_ref[pl.ds(slot * FEAT + FEAT - 1, parts, stride=SEND_ROWS), :] = jnp.full((parts, width), penalty, jnp.float32)

    wanted = ghosts_ref[...]
    entries = wanted.shape[1]
    part_of = lax.broadcasted_iota(jnp.int32, (parts, entries), 0)
    entry = lax.broadcasted_iota(jnp.int32, (parts, entries), 1)
    holder = wanted // blocks
    local_row = wanted - holder * blocks
    held = part_of == holder
    first = jnp.min(jnp.where(held, entry, entries), axis=1, keepdims=True)
    last = jnp.max(jnp.where(held, entry, -1), axis=1, keepdims=True)
    row_first = jnp.sum(jnp.where(held & (entry == first), local_row, 0), axis=1, keepdims=True)
    row_last = jnp.sum(jnp.where(held & (entry == last), local_row, 0), axis=1, keepdims=True)
    lane = lax.broadcasted_iota(jnp.int32, (parts, width), 1)
    request = jnp.where(lane == 0, row_first, jnp.where(lane == 1, row_last, 0))
    out_ref[pl.ds(OWN_ROWS, parts, stride=SEND_ROWS), :] = request.astype(jnp.float32)

    fetches[2].wait()
    ax, ay, az, bx, by, bz, cx, cy, cz, nx, ny, nz = [facets_ref[i] for i in range(12)]
    third = 1.0 / 3.0
    squares = lambda u, v, w: u * u + v * v + w * w
    spread = (squares(ax, bx, cx) + squares(ay, by, cy) + squares(az, bz, cz)) * third
    offset = spread - (nx * ax + ny * ay + nz * az)
    feats = [n - (2.0 * third) * (a + b + c) for n, a, b, c in ((nx, ax, bx, cx), (ny, ay, by, cy), (nz, az, bz, cz))]
    feats.append(offset)
    for c in range(FEAT):
        table_ref[pl.ds(c, blocks, stride=FEAT), :] = feats[c]
    for b in range(blocks):
        out_ref[pl.ds(starts[b], FEAT), :] = table_ref[b * FEAT : (b + 1) * FEAT, :]


def select_kernel(arrived_ref, table_ref, out_hbm, rows_ref, sems):
    parts = arrived_ref.shape[0] // SEND_ROWS
    request = arrived_ref[pl.ds(OWN_ROWS, parts, stride=SEND_ROWS), :].astype(jnp.int32) * FEAT
    pieces = sems.shape[0]
    share = parts // pieces
    sends = []
    for piece in range(pieces):
        for d in range(piece * share, (piece + 1) * share):
            for s in range(GC):
                row = d * REPLY_ROWS + s * FEAT
                rows_ref[row : row + FEAT, :] = table_ref[pl.ds(pl.multiple_of(request[d, s], FEAT), FEAT), :]
        here = pl.ds(piece * share * REPLY_ROWS, share * REPLY_ROWS)
        sends.append(pltpu.make_async_copy(rows_ref.at[here], out_hbm.at[here], sems.at[piece]))
        sends[-1].start()
    for send in sends:
        send.wait()


def stack_terms(high, middle, low):
    return [high, high, high, middle, middle, low]


def point_terms(points):
    four = jnp.concatenate([points, jnp.ones_like(points[0:1])], axis=0)
    high, middle, low = [t.astype(jnp.float32) for t in split3(jnp.concatenate([four, four], axis=0))]
    return [high, middle, low, high, middle, high]


def prep_kernel(limit_ref, wanted_ref, nodes_ref, cand_ref, left_ref, right_ref, spread_ref, shade_ref, place_ref, *, blocks):
    count = nodes_ref.shape[1]
    _, spread_count, width = spread_ref.shape
    start = count - spread_count
    entries = wanted_ref.shape[1]
    holder = wanted_ref[...] // blocks
    row_id = lax.broadcasted_iota(jnp.int32, (entries, entries), 0)
    col_id = lax.broadcasted_iota(jnp.int32, (entries, entries), 1)
    holder_col = jnp.sum(jnp.where(row_id == col_id, holder, 0), axis=1, keepdims=True)
    earlier = (holder_col == holder) & (row_id < col_id)
    order = jnp.sum(jnp.where(earlier, 1, 0), axis=0, keepdims=True)
    place_ref[0:1, :] = holder * REPLY_ROWS
    place_ref[1:2, :] = order
    entry = lax.broadcasted_iota(jnp.int32, (entries, count), 0)
    chosen = entry == cand_ref[0:1, :]
    for k in range(1, cand_ref.shape[0]):
        chosen = chosen | (entry == cand_ref[k : k + 1, :])
    mask = jnp.where(chosen & (entry < limit_ref[0]), 0.0, penalty)
    right = jnp.concatenate(point_terms(nodes_ref[...]) + [mask], axis=0)
    right_ref[...] = right.astype(jnp.bfloat16)
    left_ref[...] = right.T.astype(jnp.bfloat16)
    shade_ref[...] = mask[:, start:].T
    for c in range(3):
        for g in range(spread_count // width):
            row = nodes_ref[c : c + 1, start + g * width : start + (g + 1) * width]
            spread_ref[c, g * width : (g + 1) * width, :] = jnp.broadcast_to(row, (width, width)).T


def own_kernel(arrived_ref, left_ref, spread_ref, out_ref, best_ref):
    parts = arrived_ref.shape[0] // SEND_ROWS
    width = arrived_ref.shape[1]
    count = left_ref.shape[0]
    first = count - spread_ref.shape[1]
    entries = left_ref.shape[1] - 6 * 2 * FEAT
    best_ref[...] = jnp.full((count, width), penalty, jnp.float32)
    sublane = lax.broadcasted_iota(jnp.int32, (2 * FEAT, width), 0)
    chunk = CHUNK
    unroll = UNROLL

    def some_sources(i, carry):
        for u in range(unroll):
            base = (i * unroll + u) * SEND_ROWS
            sides = []
            for t in range(CAP // 2):
                tile = arrived_ref[pl.ds(base + t * 2 * FEAT, 2 * FEAT), :]
                for part in range(2):
                    kept = jnp.where((sublane >= FEAT) == (part == 1), tile, 0.0)
                    rows = stack_terms(*split3(kept)) + [jnp.zeros((entries, width), jnp.bfloat16)]
                    sides.append(jnp.concatenate(rows, axis=0))
            gaps = jnp.dot(left_ref[0:first, :], jnp.concatenate(sides, axis=1), preferred_element_type=jnp.float32)
            least = best_ref[0:first, :]
            for s in range(CAP):
                least = jnp.minimum(least, gaps[:, s * width : (s + 1) * width])
            best_ref[0:first, :] = least
            for j in range((count - first) // chunk):
                x, y, z = [spread_ref[c, j * chunk : (j + 1) * chunk, :] for c in range(3)]
                here = slice(first + j * chunk, first + (j + 1) * chunk)
                least = best_ref[here, :]
                for s in range(CAP):
                    lx, ly, lz, off = [arrived_ref[pl.ds(base + s * FEAT + c, 1), :] for c in range(FEAT)]
                    least = jnp.minimum(least, (x * lx + y * ly) + (z * lz + off))
                best_ref[here, :] = least
        return carry

    lax.fori_loop(0, parts // unroll, some_sources, 0)
    for g in range(count // width):
        here = slice(g * width, (g + 1) * width)
        out_ref[:, here] = jnp.min(best_ref[here, :].T, axis=0, keepdims=True)


def ghost_kernel(
    limit_ref, place_ref, reply_ref, nodes_ref, left_ref, right_ref, spread_ref, shade_ref, own_ref, own_out_ref, out_ref, best_ref
):
    entries = place_ref.shape[1]
    count = nodes_ref.shape[1]
    width = reply_ref.shape[1]
    spread_start = count - spread_ref.shape[1]
    first = count - GHOST_CHUNKS * CHUNK
    place = place_ref[...]
    slot = lax.broadcasted_iota(jnp.int32, (2 * FEAT, width), 0) // FEAT
    choice = lax.broadcasted_iota(jnp.int32, (entries, width), 0)

    px, py, pz = [nodes_ref[c : c + 1, :] for c in range(3)]
    square = px * px + py * py + pz * pz
    own_out_ref[...] = own_ref[...] + square

    def few_entries(members):
        best = []
        for e in members:
            tile = reply_ref[pl.ds(pl.multiple_of(place[0, e], REPLY_ROWS), REPLY_ROWS), :]
            kept = jnp.where(slot == place[1, e], tile, 0.0)
            rows = jnp.concatenate(stack_terms(*split3(kept)) + [to_one(choice == e).astype(jnp.bfloat16)], axis=0)
            gaps = jnp.dot(rows.T, right_ref[...], preferred_element_type=jnp.float32)
            best.append(jnp.min(gaps.reshape(width // 8, 8, count), axis=0))
        least = jnp.min(functools.reduce(jnp.minimum, best), axis=0, keepdims=True)
        out_ref[...] = jnp.minimum(far_gap, least + square)

    def some_entries(members):
        sides = []
        starts = []
        for e in members:
            start, order = place[0, e], place[1, e]
            starts.append(start + order * FEAT)
            tile = reply_ref[pl.ds(pl.multiple_of(start, REPLY_ROWS), REPLY_ROWS), :]
            kept = jnp.where(slot == order, tile, 0.0)
            rows = stack_terms(*split3(kept)) + [to_one(choice == e).astype(jnp.bfloat16)]
            sides.append(jnp.concatenate(rows, axis=0))
        gaps = jnp.dot(left_ref[0:first, :], jnp.concatenate(sides, axis=1), preferred_element_type=jnp.float32)
        best_ref[0:first, :] = functools.reduce(
            jnp.minimum, [gaps[:, i * width : (i + 1) * width] for i in range(len(sides))]
        )
        for j in range(first, count, CHUNK):
            here = slice(j - spread_start, j - spread_start + CHUNK)
            x, y, z = [spread_ref[c, here, :] for c in range(3)]
            least = jnp.full((CHUNK, width), penalty, jnp.float32)
            for e, start in zip(members, starts):
                lx, ly, lz, off = [reply_ref[pl.ds(start + c, 1), :] for c in range(FEAT)]
                shade = jnp.broadcast_to(shade_ref[here, e : e + 1], (CHUNK, width))
                least = jnp.minimum(least, ((x * lx + y * ly) + (z * lz + off)) + shade)
            best_ref[j : j + CHUNK, :] = least
        for g in range(count // width):
            here = slice(g * width, (g + 1) * width)
            least = jnp.min(best_ref[here, :].T, axis=0, keepdims=True)
            out_ref[:, here] = jnp.minimum(far_gap, least + square[:, here])

    least = 0
    for most in GHOST_LEVELS:
        some = min(most, entries)
        if some > least:
            fits = limit_ref[0] > least if some == entries else limit_ref[0] <= some
            pl.when(fits if least == 0 else fits & (limit_ref[0] > least))(
                functools.partial(few_entries if some <= FEW else some_entries, range(some))
            )
        least = some


def exchange(rows, parts):
    per_part = rows.shape[0] // parts
    shaped = rows.reshape(parts, per_part, 1, rows.shape[1])
    moved = lax.all_to_all(shaped, AXES, split_axis=0, concat_axis=0, tiled=True)
    return moved.reshape(rows.shape)


def local(facets, owner, ghosts, ghost_count, nodes, cand):
    parts = lax.axis_size(AXES)
    blocks, _, width = facets.shape
    count = nodes.shape[1]
    entries = ghosts.shape[1]
    f32 = jnp.float32
    smem = pl.BlockSpec(memory_space=pltpu.SMEM)
    vmem = pl.BlockSpec(memory_space=pltpu.VMEM)
    params = pltpu.CompilerParams(vmem_limit_bytes=16 * 1024 * 1024)
    hbm = pl.BlockSpec(memory_space=pltpu.HBM)
    outgoing, table = pl.pallas_call(
        pack_kernel,
        out_shape=(
            jax.ShapeDtypeStruct((parts * SEND_ROWS, width), f32),
            jax.ShapeDtypeStruct((blocks * FEAT, width), f32),
        ),
        in_specs=[hbm] * 3,
        out_specs=(vmem, vmem),
        scratch_shapes=[
            pltpu.VMEM((12, blocks, width), f32),
            pltpu.VMEM((1, blocks), jnp.int32),
            pltpu.VMEM((1, entries), jnp.int32),
            pltpu.SemaphoreType.DMA((3,)),
        ],
        name="pack",
        compiler_params=params,
    )(*[pltpu.with_memory_space_constraint(v, pltpu.HBM) for v in (jnp.transpose(facets, (1, 0, 2)), owner.T, ghosts)])
    arrived = exchange(outgoing, parts)
    left, right, spread, shade, place = pl.pallas_call(
        functools.partial(prep_kernel, blocks=blocks),
        out_shape=(
            jax.ShapeDtypeStruct((count, 6 * 2 * FEAT + entries), jnp.bfloat16),
            jax.ShapeDtypeStruct((6 * 2 * FEAT + entries, count), jnp.bfloat16),
            jax.ShapeDtypeStruct((3, SPREAD, width), f32),
            jax.ShapeDtypeStruct((SPREAD, entries), f32),
            jax.ShapeDtypeStruct((2, entries), jnp.int32),
        ),
        in_specs=[smem, vmem, vmem, vmem],
        out_specs=(vmem,) * 5,
        name="prep",
        compiler_params=params,
    )(ghost_count, ghosts, nodes, cand)
    answer = pl.pallas_call(
        select_kernel,
        out_shape=jax.ShapeDtypeStruct((parts * REPLY_ROWS, width), f32),
        in_specs=[vmem, vmem],
        out_specs=hbm,
        scratch_shapes=[pltpu.VMEM((parts * REPLY_ROWS, width), f32), pltpu.SemaphoreType.DMA((PIECES,))],
        name="select",
        compiler_params=params,
    )(arrived, table)
    reply = exchange(answer, parts)
    own_least = pl.pallas_call(
        own_kernel,
        out_shape=jax.ShapeDtypeStruct((1, count), f32),
        in_specs=[vmem] * 3,
        out_specs=vmem,
        scratch_shapes=[pltpu.VMEM((count, width), f32)],
        name="own",
        compiler_params=params,
        cost_estimate=pl.CostEstimate(
            flops=7 * parts * CAP * width * count, bytes_accessed=parts * SEND_ROWS * width * 4, transcendentals=0
        ),
    )(arrived, left, spread)
    own_gap, ghost_gap = pl.pallas_call(
        ghost_kernel,
        out_shape=[jax.ShapeDtypeStruct((1, count), f32)] * 2,
        in_specs=[smem] + [vmem] * 8,
        out_specs=[vmem, vmem],
        scratch_shapes=[pltpu.VMEM((count, width), f32)],
        name="ghost",
        compiler_params=params,
    )(ghost_count, place, reply, nodes, left, right, spread, shade, own_least)
    return own_gap.reshape(count), ghost_gap.reshape(count)


def solution(mesh):
    return jax.shard_map(
        local,
        mesh=mesh,
        in_specs=(
            P(AXES, None, None),
            P(AXES, None),
            P(AXES, None),
            P(AXES),
            P(None, AXES),
            P(None, AXES),
        ),
        out_specs=(P(AXES), P(AXES)),
        check_vma=False,
    )
```
